16 devices in a mesh: rep: 4 (over y, z, core), dp: 4 (over x).
Axes of the slice: x: 4, y: 2, z: 1, core: 2. Of those that a mesh axis runs over, the one named last changes fastest.
The devices are a block of a 4x4x8 slice.
Arguments:
- a: bfloat16 [16, 4, 4096, 896], P(('rep', 'dp')), parts along dimension 0
- g: bfloat16 [16, 4, 4096, 2304], P(('rep', 'dp')), parts along dimension 0
Outputs:
- output: bfloat16 [16, 896, 2304], P('rep'), parts along dimension 0
There are 4 independent parts. The reference program is written for one: setup_inputs(seed, part) draws one part's arguments, and reference() takes and returns one part's arrays. A program takes and returns all parts, laid end to end along the dimension named above; each array names one.
All inputs are finite; a program needn't handle non-finite values.
Results may differ from the reference program's by a relative error of at most 0.012.
Values are sent between devices in bfloat16 or wider.
A program may use at most 768 MiB of HBM per device.

```python
import jax
import jax.numpy as jnp
from jax import lax

DEVICES = 4
MATRICES = 4
TOKENS = 4096
D = 896
FF = 2304


def setup_inputs(seed: int = 0, part: int = 0) -> dict:
    ka, kg, ks = (jax.random.fold_in(k, part) for k in jax.random.split(jax.random.key(seed), 3))
    size = 2.0 ** jax.random.uniform(ks, (DEVICES, MATRICES, 1, 1), jnp.float32, -1.0, 1.0)
    a = jax.random.normal(ka, (DEVICES, MATRICES, TOKENS, D), jnp.float32)
    g = size * jax.random.normal(kg, (DEVICES, MATRICES, TOKENS, FF), jnp.float32) * (DEVICES * TOKENS) ** -0.5
    return {"a": a.astype(jnp.bfloat16), "g": g.astype(jnp.bfloat16)}


def reference(a, g):
    def take(so_far, one):
        return so_far + jnp.einsum("ntd,ntf->ndf", *one, preferred_element_type=jnp.float32), None

    return lax.scan(take, jnp.zeros((MATRICES, D, FF), jnp.float32), (a, g))[0].astype(jnp.bfloat16)
```

```python
import jax
import jax.numpy as jnp
from jax import lax
from jax.sharding import PartitionSpec as P


def solution(mesh):
    def local(a, g):
        outs = []
        for n in range(a.shape[1]):
            part = lax.dot_general(
                a[0, n], g[0, n], (((0,), (0,)), ((), ())), preferred_element_type=jnp.float32
            ).astype(jnp.bfloat16)
            if outs:
                part, outs[-1] = lax.optimization_barrier((part, outs[-1]))
            outs.append(lax.psum(part, "dp"))
        return jnp.stack(outs)

    return jax.shard_map(
        local,
        mesh=mesh,
        in_specs=(P(("rep", "dp")), P(("rep", "dp"))),
        out_specs=P("rep"),
        check_vma=False,
    )
```

```python
import functools

import jax
import jax.numpy as jnp
from jax import lax
from jax.experimental import pallas as pl
from jax.experimental.pallas import tpu as pltpu
from jax.sharding import PartitionSpec as P

MESH = pl.DeviceIdType.MESH
WIDTH = 256
LAG = 8
FWD = 3
ACC = 4
SEND = 4


def kernel(per, pieces, a_ref, g_ref, o_ref, a_buf, g_buf, acc, sb1, sb2, r1, r2, fin,
           a_sem, g_sem, s1s, s1r, s2s, s2r, ags, agr, fws, fwr, los):
    n = 4
    me = lax.axis_index("dp")
    right, left, opp = lax.rem(me + 1, n), lax.rem(me + 3, n), lax.rem(me + 2, n)
    sides = (right, left)
    rows = fin.shape[1]
    half = rows // 2

    def rows_of(owner, h=None):
        start = owner * rows + (0 if h is None else h * half)
        return pl.ds(pl.multiple_of(start, 16), rows if h is None else half)

    def cols(q):
        return pl.ds(pl.multiple_of(q * WIDTH, WIDTH), WIDTH)

    def split(p):
        return lax.div(p, per), lax.rem(p, per)

    def load_a(m):
        return pltpu.make_async_copy(a_ref.at[0, m], a_buf.at[lax.rem(m, 2)], a_sem.at[lax.rem(m, 2)])

    def load_g(p):
        m, q = split(p)
        slot = lax.rem(p, 3)
        return pltpu.make_async_copy(g_ref.at[0, m, :, cols(q)], g_buf.at[slot], g_sem.at[slot])

    def remote(src, dst, ss, rs, d):
        return pltpu.make_async_remote_copy(
            src_ref=src, dst_ref=dst, send_sem=ss, recv_sem=rs, device_id={"dp": sides[d]}, device_id_type=MESH
        )

    def send1(p, d):
        slot = lax.rem(p, SEND)
        return remote(sb1.at[slot, d], r1.at[p, d], s1s.at[slot, d], s1r.at[p, d], d)

    def send2(p, d):
        slot = lax.rem(p, SEND)
        return remote(sb2.at[slot, d], r2.at[p, d], s2s.at[slot, d], s2r.at[p, d], d)

    def out(p, owner, h=None):
        m, q = split(p)
        return o_ref.at[m, rows_of(owner, h), cols(q)]

    def gather(p, d):
        return remote(fin.at[p], out(p, me), ags.at[p, d], agr.at[p, d], d)

    def forward(p, d):
        block = out(p, (left, right)[d], d)
        return remote(block, block, fws.at[p, d], fwr.at[p, d], d)

    def local(p):
        return pltpu.make_async_copy(fin.at[p], out(p, me), los.at[p])

    load_a(0).start()
    load_g(0).start()
    load_g(1).start()

    barrier = pltpu.get_barrier_semaphore()
    for d in sides:
        pl.semaphore_signal(barrier, inc=1, device_id={"dp": d}, device_id_type=MESH)

    def step(i, carry):
        @pl.when(i < pieces)
        def _():
            m, q = split(i)
            slot, mine = lax.rem(i, SEND), lax.rem(i, ACC)

            @pl.when(q == 0)
            def _():
                load_a(m).wait()

                @pl.when(i + per < pieces)
                def _():
                    load_a(m + 1).start()

            load_g(i).wait()

            @pl.when(i + 2 < pieces)
            def _():
                load_g(i + 2).start()

            acc[mine] = lax.dot_general(
                a_buf[lax.rem(m, 2)], g_buf[lax.rem(i, 3)], (((0,), (0,)), ((), ())),
                preferred_element_type=jnp.float32,
            )

            @pl.when(i == 0)
            def _():
                pl.semaphore_wait(barrier, 2)

            @pl.when(i >= SEND)
            def _():
                for d in range(2):
                    send1(i - SEND, d).wait_send()

            for d in range(2):
                sb1[slot, d, :half] = acc[mine, rows_of(opp, d)].astype(jnp.bfloat16)
                sb1[slot, d, half:] = acc[mine, rows_of(sides[d], 1 - d)].astype(jnp.bfloat16)
            for d in range(2):
                send1(i, d).start()

        @pl.when((i >= 1) & (i < pieces + 1))
        def _():
            p = i - 1
            slot, mine = lax.rem(p, SEND), lax.rem(p, ACC)

            @pl.when(p >= SEND)
            def _():
                for d in range(2):
                    send2(p - SEND, d).wait_send()

            for d in range(2):
                send1(p, d).wait_recv()
                sb2[slot, d] = (
                    acc[mine, rows_of(sides[d], d)] + r1[p, d, :half].astype(jnp.float32)
                ).astype(jnp.bfloat16)
                send2(p, d).start()

        @pl.when((i >= 2) & (i < pieces + 2))
        def _():
            p = i - 2
            mine = lax.rem(p, ACC)
            for d in range(2):
                send2(p, d).wait_recv()
                fin[p, d * half:(d + 1) * half] = (
                    acc[mine, rows_of(me, d)]
                    + r2[p, d].astype(jnp.float32)
                    + r1[p, 1 - d, half:].astype(jnp.float32)
                ).astype(jnp.bfloat16)
            local(p).start()

        @pl.when((i >= 2 + LAG) & (i < pieces + 2 + LAG))
        def _():
            for d in range(2):
                gather(i - 2 - LAG, d).start()

        @pl.when(i >= 2 + LAG + FWD)
        def _():
            p = i - 2 - LAG - FWD
            for d in range(2):
                gather(p, d).wait_recv()
                forward(p, d).start()

        return carry

    lax.fori_loop(0, pieces + 2 + LAG + FWD, step, 0)

    def drain(p, carry):
        local(p).wait()
        for d in range(2):
            gather(p, d).wait_send()
            forward(p, d).wait()
        return carry

    lax.fori_loop(0, pieces, drain, 0)
    for p in range(pieces - SEND, pieces):
        for d in range(2):
            send1(p, d).wait_send()
            send2(p, d).wait_send()


def solution(mesh):
    def local(a, g):
        _, count, tokens, d = a.shape
        ff = g.shape[3]
        per = ff // WIDTH
        pieces = count * per
        rows = d // mesh.shape["dp"]
        dma = pltpu.SemaphoreType.DMA
        bf16 = jnp.bfloat16
        return pl.pallas_call(
            functools.partial(kernel, per, pieces),
            out_shape=jax.ShapeDtypeStruct((count, d, ff), bf16),
            in_specs=[pl.BlockSpec(memory_space=pltpu.HBM)] * 2,
            out_specs=pl.BlockSpec(memory_space=pltpu.HBM),
            scratch_shapes=[
                pltpu.VMEM((2, tokens, d), bf16),
                pltpu.VMEM((3, tokens, WIDTH), bf16),
                pltpu.VMEM((ACC, d, WIDTH), jnp.float32),
                pltpu.VMEM((SEND, 2, rows, WIDTH), bf16),
                pltpu.VMEM((SEND, 2, rows // 2, WIDTH), bf16),
                pltpu.VMEM((pieces, 2, rows, WIDTH), bf16),
                pltpu.VMEM((pieces, 2, rows // 2, WIDTH), bf16),
                pltpu.VMEM((pieces, rows, WIDTH), bf16),
                dma((2,)),
                dma((3,)),
                dma((SEND, 2)),
                dma((pieces, 2)),
                dma((SEND, 2)),
                dma((pieces, 2)),
                dma((pieces, 2)),
                dma((pieces, 2)),
                dma((pieces, 2)),
                dma((pieces, 2)),
                dma((pieces,)),
            ],
            compiler_params=pltpu.CompilerParams(
                collective_id=0, has_side_effects=True, vmem_limit_bytes=60 * 1024 * 1024
            ),
            name="sums",
        )(a, g)

    return jax.shard_map(
        local,
        mesh=mesh,
        in_specs=(P(("rep", "dp")), P(("rep", "dp"))),
        out_specs=P("rep"),
        check_vma=False,
    )
```

```python
import functools

import jax
import jax.numpy as jnp
from jax import lax
from jax.experimental import pallas as pl
from jax.experimental.pallas import tpu as pltpu
from jax.sharding import PartitionSpec as P

MESH = pl.DeviceIdType.MESH
BF16 = jnp.bfloat16
WIDTH = 256
GROUP = 3
FIRST = 4
T1, T2, T3, T4 = 2, 3, 5, 6
EVERY, OFFSET = 4, 8
FWD = 3
ACC, V1, V2, SEND = T4 + 1, T4 - T1 + 1, T4 - T3 + 1, 4


def sums_kernel(per, pieces, a_ref, g_ref, res, land, h1, h2, a_buf, g_buf, acc, sb1, sb2, v1, v2,
                a_sem, g_sem, f_sem, s1s, s1r, s2s, s2r, l1, l2, ags, agr, fws, fwr, lon, lof):
    n = 4
    me = lax.axis_index("dp")
    right, left, opp = lax.rem(me + 1, n), lax.rem(me + 3, n), lax.rem(me + 2, n)
    sides = (right, left)
    rows = h1.shape[2]
    half = rows // 2
    groups = pieces // GROUP
    chunk = a_buf.shape[1] // FIRST

    def rows_of(owner, h=None):
        start = owner * rows + (0 if h is None else h * half)
        return pl.ds(pl.multiple_of(start, 16), rows if h is None else half)

    def block(ref, p, width, owner, h=None):
        m, q = lax.div(p, per), lax.rem(p, per)
        return ref.at[m, rows_of(owner, h), pl.ds(pl.multiple_of(q * WIDTH, WIDTH), width)]

    def load_a(m):
        return pltpu.make_async_copy(a_ref.at[0, m], a_buf.at[lax.rem(m, 2)], a_sem.at[lax.rem(m, 2)])

    def load_g(p):
        m, q = lax.div(p, per), lax.rem(p, per)
        slot = lax.rem(p, 3)
        cols = pl.ds(pl.multiple_of(q * WIDTH, WIDTH), WIDTH)
        return pltpu.make_async_copy(g_ref.at[0, m, :, cols], g_buf.at[slot], g_sem.at[slot])

    def first(k):
        t = pl.ds(pl.multiple_of(k * chunk, chunk), chunk)
        return (
            pltpu.make_async_copy(g_ref.at[0, 0, t, pl.ds(0, WIDTH)], g_buf.at[0, t], f_sem.at[k, 0]),
            pltpu.make_async_copy(a_ref.at[0, 0, t], a_buf.at[0, t], f_sem.at[k, 1]),
        )

    def remote(src, dst, ss, rs, d):
        return pltpu.make_async_remote_copy(
            src_ref=src, dst_ref=dst, send_sem=ss, recv_sem=rs, device_id={"dp": sides[d]}, device_id_type=MESH
        )

    def send1(p, d):
        slot = lax.rem(p, SEND)
        return remote(sb1.at[slot, d], h1.at[p, d], s1s.at[slot, d], s1r.at[p, d], d)

    def send2(p, d):
        slot = lax.rem(p, SEND)
        return remote(sb2.at[slot, d], h2.at[p, d], s2s.at[slot, d], s2r.at[p, d], d)

    def load1(p, d):
        slot = lax.rem(p, V1)
        return pltpu.make_async_copy(h1.at[p, d], v1.at[slot, d], l1.at[slot, d])

    def load2(p, d):
        slot = lax.rem(p, V2)
        return pltpu.make_async_copy(h2.at[p, d], v2.at[slot, d], l2.at[slot, d])

    def gather(k, d):
        p, width = k * GROUP, GROUP * WIDTH
        return remote(block(res, p, width, me), block(land, p, width, me), ags.at[k, d], agr.at[k, d], d)

    def forward(k, d):
        b = block(land, k * GROUP, GROUP * WIDTH, (left, right)[d], d)
        return remote(b, b, fws.at[k, d], fwr.at[k, d], d)

    def keep_near(k, d):
        p, width, owner = k * GROUP, GROUP * WIDTH, (left, right)[d]
        return pltpu.make_async_copy(block(land, p, width, owner), block(res, p, width, owner), lon.at[k, d])

    def keep_far(k, d):
        p, width = k * GROUP, GROUP * WIDTH
        return pltpu.make_async_copy(block(land, p, width, opp, d), block(res, p, width, opp, d), lof.at[k, d])

    def gather_start(k):
        for d in range(2):
            gather(k, d).start()

    def forward_start(k):
        for d in range(2):
            gather(k, d).wait_recv()
            forward(k, d).start()
            keep_near(k, d).start()

    def far_start(k):
        for d in range(2):
            forward(k, d).wait_recv()
            keep_far(k, d).start()

    for k in range(FIRST):
        for copy in first(k):
            copy.start()
    load_g(1).start()

    barrier = pltpu.get_barrier_semaphore()
    for d in sides:
        pl.semaphore_signal(barrier, inc=1, device_id={"dp": d}, device_id_type=MESH)

    def product(lhs, rhs):
        return lax.dot_general(lhs, rhs, (((0,), (0,)), ((), ())), preferred_element_type=jnp.float32)

    acc[0] = jnp.zeros_like(acc[0])

    def first_step(k, carry):
        for copy in first(k):
            copy.wait()
        t = pl.ds(pl.multiple_of(k * chunk, chunk), chunk)
        acc[0] += product(a_buf[0, t], g_buf[0, t])
        return carry

    lax.fori_loop(0, FIRST, first_step, 0)
    pl.semaphore_wait(barrier, 2)

    def step(i, carry):
        @pl.when(i < pieces)
        def _():
            m, q = lax.div(i, per), lax.rem(i, per)
            slot, mine = lax.rem(i, SEND), lax.rem(i, ACC)

            @pl.when(i + 2 < pieces)
            def _():
                load_g(i + 2).start()

            @pl.when((q == 0) & (i + per < pieces))
            def _():
                load_a(m + 1).start()

            @pl.when(i > 0)
            def _():
                @pl.when(q == 0)
                def _():
                    load_a(m).wait()

                load_g(i).wait()
                acc[mine] = product(a_buf[lax.rem(m, 2)], g_buf[lax.rem(i, 3)])

            @pl.when(i >= SEND)
            def _():
                for d in range(2):
                    send1(i - SEND, d).wait_send()

            for d in range(2):
                sb1[slot, d, :half] = acc[mine, rows_of(opp, d)].astype(BF16)
                sb1[slot, d, half:] = acc[mine, rows_of(sides[d], 1 - d)].astype(BF16)
            for d in range(2):
                send1(i, d).start()

        @pl.when((i >= T1) & (i < pieces + T1))
        def _():
            for d in range(2):
                send1(i - T1, d).wait_recv()
                load1(i - T1, d).start()

        @pl.when((i >= T2) & (i < pieces + T2))
        def _():
            p = i - T2
            slot, mine, here = lax.rem(p, SEND), lax.rem(p, ACC), lax.rem(p, V1)

            @pl.when(p >= SEND)
            def _():
                for d in range(2):
                    send2(p - SEND, d).wait_send()

            for d in range(2):
                load1(p, d).wait()
                sb2[slot, d] = (acc[mine, rows_of(sides[d], d)] + v1[here, d, :half].astype(jnp.float32)).astype(BF16)
            for d in range(2):
                send2(p, d).start()

        @pl.when((i >= T3) & (i < pieces + T3))
        def _():
            for d in range(2):
                send2(i - T3, d).wait_recv()
                load2(i - T3, d).start()

        @pl.when(i >= T4)
        def _():
            p = i - T4
            m, q = lax.div(p, per), lax.rem(p, per)
            mine, one, two = lax.rem(p, ACC), lax.rem(p, V1), lax.rem(p, V2)
            cols = pl.ds(pl.multiple_of(q * WIDTH, WIDTH), WIDTH)
            for d in range(2):
                load2(p, d).wait()
                res[m, rows_of(me, d), cols] = (
                    acc[mine, rows_of(me, d)]
                    + v2[two, d].astype(jnp.float32)
                    + v1[one, 1 - d, half:].astype(jnp.float32)
                ).astype(BF16)

        t = i - OFFSET

        @pl.when((t >= 0) & (lax.rem(t, EVERY) == 0))
        def _():
            gather_start(lax.div(t, EVERY))

        @pl.when((t >= FWD) & (lax.rem(t - FWD, EVERY) == 0))
        def _():
            k = lax.div(t - FWD, EVERY)
            forward_start(k)

            @pl.when(k >= 2)
            def _():
                far_start(k - 2)

        return carry

    last = pieces + T4
    lax.fori_loop(0, last, step, 0)

    def over(f, start, stop):
        def body(k, carry):
            f(k)
            return carry

        lax.fori_loop(start, stop, body, 0)

    gathered = (last - 1 - OFFSET) // EVERY + 1
    forwarded = (last - 1 - OFFSET - FWD) // EVERY + 1
    over(gather_start, gathered, groups)
    over(forward_start, forwarded, groups)
    over(far_start, max(forwarded - 2, 0), groups)

    def drain(k):
        for d in range(2):
            gather(k, d).wait_send()
            forward(k, d).wait_send()
            keep_near(k, d).wait()
            keep_far(k, d).wait()

    for p in range(pieces - SEND, pieces):
        for d in range(2):
            send1(p, d).wait_send()
            send2(p, d).wait_send()
    over(drain, 0, groups)


def write_kernel(res, o_ref, sem):
    count = res.shape[0]
    copies = [pltpu.make_async_copy(res.at[m], o_ref.at[m], sem.at[m]) for m in range(count)]
    for copy in copies:
        copy.start()
    for copy in copies:
        copy.wait()


def solution(mesh):
    def local(a, g):
        _, count, tokens, d = a.shape
        ff = g.shape[3]
        per = ff // WIDTH
        pieces = count * per
        groups = pieces // GROUP
        rows = d // mesh.shape["dp"]
        dma = pltpu.SemaphoreType.DMA
        hbm = pl.BlockSpec(memory_space=pltpu.HBM)
        res = pl.pallas_call(
            functools.partial(sums_kernel, per, pieces),
            out_shape=(
                pltpu.VMEM((count, d, ff), BF16),
                jax.ShapeDtypeStruct((count, d, ff), BF16),
                jax.ShapeDtypeStruct((pieces, 2, rows, WIDTH), BF16),
                jax.ShapeDtypeStruct((pieces, 2, rows // 2, WIDTH), BF16),
            ),
            in_specs=[hbm] * 2,
            out_specs=(pl.BlockSpec(memory_space=pltpu.VMEM), hbm, hbm, hbm),
            scratch_shapes=[
                pltpu.VMEM((2, tokens, d), BF16),
                pltpu.VMEM((3, tokens, WIDTH), BF16),
                pltpu.VMEM((ACC, d, WIDTH), jnp.float32),
                pltpu.VMEM((SEND, 2, rows, WIDTH), BF16),
                pltpu.VMEM((SEND, 2, rows // 2, WIDTH), BF16),
                pltpu.VMEM((V1, 2, rows, WIDTH), BF16),
                pltpu.VMEM((V2, 2, rows // 2, WIDTH), BF16),
                dma((2,)),
                dma((3,)),
                dma((FIRST, 2)),
                dma((SEND, 2)),
                dma((pieces, 2)),
                dma((SEND, 2)),
                dma((pieces, 2)),
                dma((V1, 2)),
                dma((V2, 2)),
                dma((groups, 2)),
                dma((groups, 2)),
                dma((groups, 2)),
                dma((groups, 2)),
                dma((groups, 2)),
                dma((groups, 2)),
            ],
            compiler_params=pltpu.CompilerParams(
                collective_id=0, has_side_effects=True, vmem_limit_bytes=40 * 1024 * 1024
            ),
            name="sums",
        )(a, g)[0]
        return pl.pallas_call(
            write_kernel,
            out_shape=jax.ShapeDtypeStruct((count, d, ff), BF16),
            in_specs=[pl.BlockSpec(memory_space=pltpu.VMEM)],
            out_specs=hbm,
            scratch_shapes=[dma((count,))],
            compiler_params=pltpu.CompilerParams(vmem_limit_bytes=4 * 1024 * 1024),
            name="write",
        )(res)

    return jax.shard_map(
        local,
        mesh=mesh,
        in_specs=(P(("rep", "dp")), P(("rep", "dp"))),
        out_specs=P("rep"),
        check_vma=False,
    )
```

```python
import functools

import jax
import jax.numpy as jnp
from jax import lax
from jax.experimental import pallas as pl
from jax.experimental.pallas import tpu as pltpu
from jax.sharding import PartitionSpec as P

MESH = pl.DeviceIdType.MESH
BF16 = jnp.bfloat16
WIDTH = 256
GROUP = 3
FIRST = 4
T1, T2, T3, T4 = 3, 4, 6, 7
EVERY, OFFSET = 4, 9
PARTS = 4
FWD = 3
ACC, V1, V2, SEND = T4 + 1, T4 - T1 + 1, T4 - T3 + 1, 4
RECV = 8
KEEP = 4


def sums_kernel(per, pieces, a_ref, g_ref, res, land, h1, h2, a_buf, g_buf, acc, sb1, sb2, v1, v2,
                a_sem, g_sem, f_sem, s1s, s1r, s2s, s2r, l1, l2, ags, agr, fws, fwr, lon, lof):
    n = 4
    me = lax.axis_index("dp")
    right, left, opp = lax.rem(me + 1, n), lax.rem(me + 3, n), lax.rem(me + 2, n)
    sides = (right, left)
    rows = h1.shape[2]
    half = rows // 2
    groups = pieces // GROUP
    chunk = a_buf.shape[1] // FIRST

    def rows_of(owner, h=None):
        start = owner * rows + (0 if h is None else h * half)
        return pl.ds(pl.multiple_of(start, 16), rows if h is None else half)

    def block(ref, p, width, owner, h=None):
        m, q = lax.div(p, per), lax.rem(p, per)
        return ref.at[m, rows_of(owner, h), pl.ds(pl.multiple_of(q * WIDTH, WIDTH), width)]

    def load_a(m):
        return pltpu.make_async_copy(a_ref.at[0, m], a_buf.at[lax.rem(m, 2)], a_sem.at[lax.rem(m, 2)])

    def load_g(p):
        m, q = lax.div(p, per), lax.rem(p, per)
        slot = lax.rem(p, 3)
        cols = pl.ds(pl.multiple_of(q * WIDTH, WIDTH), WIDTH)
        return pltpu.make_async_copy(g_ref.at[0, m, :, cols], g_buf.at[slot], g_sem.at[slot])

    def first(k):
        t = pl.ds(pl.multiple_of(k * chunk, chunk), chunk)
        return (
            pltpu.make_async_copy(g_ref.at[0, 0, t, pl.ds(0, WIDTH)], g_buf.at[0, t], f_sem.at[k, 0]),
            pltpu.make_async_copy(a_ref.at[0, 0, t], a_buf.at[0, t], f_sem.at[k, 1]),
        )

    def remote(src, dst, ss, rs, d):
        return pltpu.make_async_remote_copy(
            src_ref=src, dst_ref=dst, send_sem=ss, recv_sem=rs, device_id={"dp": sides[d]}, device_id_type=MESH
        )

    def send1(p, d):
        slot = lax.rem(p, SEND)
        return remote(sb1.at[slot, d], h1.at[p, d], s1s.at[slot, d], s1r.at[lax.rem(p, RECV), d], d)

    def send2(p, d):
        slot = lax.rem(p, SEND)
        return remote(sb2.at[slot, d], h2.at[p, d], s2s.at[slot, d], s2r.at[lax.rem(p, RECV), d], d)

    def load1(p, d):
        slot = lax.rem(p, V1)
        return pltpu.make_async_copy(h1.at[p, d], v1.at[slot, d], l1.at[slot, d])

    def load2(p, d):
        slot = lax.rem(p, V2)
        return pltpu.make_async_copy(h2.at[p, d], v2.at[slot, d], l2.at[slot, d])

    def gather(k, d):
        b = block(land, k * GROUP, GROUP * WIDTH, me)
        return remote(block(res, k * GROUP, GROUP * WIDTH, me), b, ags.at[lax.rem(k, KEEP), d], agr.at[k, d], d)

    def forward(k, d, to):
        p, width, owner = k * GROUP, GROUP * WIDTH, (left, right)[d]
        return remote(
            block(land, p, width, owner, d), block(to, p, width, owner, d), fws.at[lax.rem(k, KEEP), d], fwr.at[k, d], d
        )

    def keep_near(k, d):
        p, width, owner = k * GROUP, GROUP * WIDTH, (left, right)[d]
        return pltpu.make_async_copy(
            block(land, p, width, owner), block(res, p, width, owner), lon.at[lax.rem(k, KEEP), d]
        )

    def keep_far(k, d):
        p, width = k * GROUP, GROUP * WIDTH
        return pltpu.make_async_copy(
            block(land, p, width, opp, d), block(res, p, width, opp, d), lof.at[lax.rem(k, KEEP), d]
        )

    def gather_start(k):
        @pl.when(k >= KEEP)
        def _():
            for d in range(2):
                gather(k - KEEP, d).wait_send()

        for d in range(2):
            gather(k, d).start()

    def forward_start(k, to=land):
        @pl.when(k >= KEEP)
        def _():
            for d in range(2):
                forward(k - KEEP, d, land).wait_send()
                keep_near(k - KEEP, d).wait()

        for d in range(2):
            gather(k, d).wait_recv()
            forward(k, d, to).start()
            keep_near(k, d).start()

    def far_start(k):
        @pl.when(k >= KEEP)
        def _():
            for d in range(2):
                keep_far(k - KEEP, d).wait()

        for d in range(2):
            forward(k, d, land).wait_recv()
            keep_far(k, d).start()

    for k in range(FIRST):
        for copy in first(k):
            copy.start()

    barrier = pltpu.get_barrier_semaphore()
    for d in sides:
        pl.semaphore_signal(barrier, inc=1, device_id={"dp": d}, device_id_type=MESH)

    def product(lhs, rhs):
        return lax.dot_general(lhs, rhs, (((0,), (0,)), ((), ())), preferred_element_type=jnp.float32)

    acc[0] = jnp.zeros_like(acc[0])

    def first_step(k, carry):
        for copy in first(k):
            copy.wait()
        t = pl.ds(pl.multiple_of(k * chunk, chunk), chunk)

        @pl.when(k == FIRST - 1)
        def _():
            load_g(1).start()

        acc[0] += product(a_buf[0, t], g_buf[0, t])
        return carry

    lax.fori_loop(0, FIRST, first_step, 0)
    pl.semaphore_wait(barrier, 2)

    def step(i, carry):
        @pl.when(i < pieces)
        def _():
            m, q = lax.div(i, per), lax.rem(i, per)
            slot, mine = lax.rem(i, SEND), lax.rem(i, ACC)

            @pl.when(i + 2 < pieces)
            def _():
                load_g(i + 2).start()

            @pl.when((q == 0) & (i + per < pieces))
            def _():
                load_a(m + 1).start()

            @pl.when(i > 0)
            def _():
                @pl.when(q == 0)
                def _():
                    load_a(m).wait()

                load_g(i).wait()
                acc[mine] = product(a_buf[lax.rem(m, 2)], g_buf[lax.rem(i, 3)])

            @pl.when(i >= SEND)
            def _():
                for d in range(2):
                    send1(i - SEND, d).wait_send()

            for d in range(2):
                sb1[slot, d, :half] = acc[mine, rows_of(opp, d)].astype(BF16)
                sb1[slot, d, half:] = acc[mine, rows_of(sides[d], 1 - d)].astype(BF16)
            for d in range(2):
                send1(i, d).start()

        @pl.when((i >= T1) & (i < pieces + T1))
        def _():
            for d in range(2):
                send1(i - T1, d).wait_recv()
                load1(i - T1, d).start()

        @pl.when((i >= T2) & (i < pieces + T2))
        def _():
            p = i - T2
            slot, mine, here = lax.rem(p, SEND), lax.rem(p, ACC), lax.rem(p, V1)

            @pl.when(p >= SEND)
            def _():
                for d in range(2):
                    send2(p - SEND, d).wait_send()

            for d in range(2):
                load1(p, d).wait()
                sb2[slot, d] = (acc[mine, rows_of(sides[d], d)] + v1[here, d, :half].astype(jnp.float32)).astype(BF16)
            for d in range(2):
                send2(p, d).start()

        @pl.when((i >= T3) & (i < pieces + T3))
        def _():
            for d in range(2):
                send2(i - T3, d).wait_recv()
                load2(i - T3, d).start()

        @pl.when(i >= T4)
        def _():
            p = i - T4
            m, q = lax.div(p, per), lax.rem(p, per)
            mine, one, two = lax.rem(p, ACC), lax.rem(p, V1), lax.rem(p, V2)
            cols = pl.ds(pl.multiple_of(q * WIDTH, WIDTH), WIDTH)
            for d in range(2):
                load2(p, d).wait()
                res[m, rows_of(me, d), cols] = (
                    acc[mine, rows_of(me, d)]
                    + v2[two, d].astype(jnp.float32)
                    + v1[one, 1 - d, half:].astype(jnp.float32)
                ).astype(BF16)

        t = i - OFFSET

        @pl.when((t >= 0) & (lax.rem(t, EVERY) == 0))
        def _():
            gather_start(lax.div(t, EVERY))

        @pl.when((t >= FWD) & (lax.rem(t - FWD, EVERY) == 0))
        def _():
            k = lax.div(t - FWD, EVERY)
            forward_start(k)

            @pl.when(k >= 2)
            def _():
                far_start(k - 2)

        return carry

    last = pieces + T4
    lax.fori_loop(0, last, step, 0)

    def over(f, start, stop):
        def body(k, carry):
            f(k)
            return carry

        lax.fori_loop(start, stop, body, 0)

    gathered = (last - 1 - OFFSET) // EVERY + 1
    forwarded = (last - 1 - OFFSET - FWD) // EVERY + 1
    final = groups - 1
    over(gather_start, gathered, groups)
    over(forward_start, forwarded, final)
    forward_start(final, res)
    over(far_start, max(forwarded - 2, 0), final)

    for p in range(pieces - SEND, pieces):
        for d in range(2):
            send1(p, d).wait_send()
            send2(p, d).wait_send()

    def drain(k):
        for d in range(2):
            gather(k, d).wait_send()
            keep_near(k, d).wait()
            forward(k, d, land).wait_send()

    def drain_far(k):
        for d in range(2):
            keep_far(k, d).wait()

    over(drain, groups - KEEP, groups)
    over(drain_far, final - KEEP, final)
    for d in range(2):
        forward(final, d, res).wait_recv()


def write_kernel(res, o_ref, sem):
    count, d, _ = res.shape
    step = d // PARTS
    copies = [
        pltpu.make_async_copy(
            res.at[m, pl.ds(k * step, step)], o_ref.at[m, pl.ds(k * step, step)], sem.at[m, k]
        )
        for m in range(count)
        for k in range(PARTS)
    ]
    for copy in copies:
        copy.start()
    for copy in copies:
        copy.wait()


def solution(mesh):
    def local(a, g):
        _, count, tokens, d = a.shape
        ff = g.shape[3]
        per = ff // WIDTH
        pieces = count * per
        groups = pieces // GROUP
        rows = d // mesh.shape["dp"]
        dma = pltpu.SemaphoreType.DMA
        hbm = pl.BlockSpec(memory_space=pltpu.HBM)
        res = pl.pallas_call(
            functools.partial(sums_kernel, per, pieces),
            out_shape=(
                pltpu.VMEM((count, d, ff), BF16),
                jax.ShapeDtypeStruct((count, d, ff), BF16),
                jax.ShapeDtypeStruct((pieces, 2, rows, WIDTH), BF16),
                jax.ShapeDtypeStruct((pieces, 2, rows // 2, WIDTH), BF16),
            ),
            in_specs=[hbm] * 2,
            out_specs=(pl.BlockSpec(memory_space=pltpu.VMEM), hbm, hbm, hbm),
            scratch_shapes=[
                pltpu.VMEM((2, tokens, d), BF16),
                pltpu.VMEM((3, tokens, WIDTH), BF16),
                pltpu.VMEM((ACC, d, WIDTH), jnp.float32),
                pltpu.VMEM((SEND, 2, rows, WIDTH), BF16),
                pltpu.VMEM((SEND, 2, rows // 2, WIDTH), BF16),
                pltpu.VMEM((V1, 2, rows, WIDTH), BF16),
                pltpu.VMEM((V2, 2, rows // 2, WIDTH), BF16),
                dma((2,)),
                dma((3,)),
                dma((FIRST, 2)),
                dma((SEND, 2)),
                dma((RECV, 2)),
                dma((SEND, 2)),
                dma((RECV, 2)),
                dma((V1, 2)),
                dma((V2, 2)),
                dma((KEEP, 2)),
                dma((groups, 2)),
                dma((KEEP, 2)),
                dma((groups, 2)),
                dma((KEEP, 2)),
                dma((KEEP, 2)),
            ],
            compiler_params=pltpu.CompilerParams(
                collective_id=0, has_side_effects=True, vmem_limit_bytes=40 * 1024 * 1024
            ),
            name="sums",
        )(a, g)[0]
        return pl.pallas_call(
            write_kernel,
            out_shape=jax.ShapeDtypeStruct((count, d, ff), BF16),
            in_specs=[pl.BlockSpec(memory_space=pltpu.VMEM)],
            out_specs=hbm,
            scratch_shapes=[dma((count, PARTS))],
            compiler_params=pltpu.CompilerParams(vmem_limit_bytes=4 * 1024 * 1024),
            name="write",
        )(res)

    return jax.shard_map(
        local,
        mesh=mesh,
        in_specs=(P(("rep", "dp")), P(("rep", "dp"))),
        out_specs=P("rep"),
        check_vma=False,
    )
```

```python
import functools

import jax
import jax.numpy as jnp
from jax import lax
from jax.experimental import pallas as pl
from jax.experimental.pallas import tpu as pltpu
from jax.sharding import PartitionSpec as P

MESH = pl.DeviceIdType.MESH
BF16 = jnp.bfloat16
WIDTH = 256
GROUP = 3
FIRST = 4
T1, T2, T3, T4 = 3, 4, 6, 7
EVERY, OFFSET = 4, 9
LATER = 2
DEEP = 3
FWD = 3
ACC, V1, V2, SEND = T4 + 1, T4 - T1 + 1, T4 - T3 + 1, 4
RECV, KEEP = 7, 4


def sums_kernel(per, pieces, a_ref, g_ref, res, land, h1, h2, a_buf, g_buf, acc, sb1, sb2, v1, v2,
                a_sem, g_sem, f_sem, s1s, s1r, s2s, s2r, l1, l2, ags, agr, fws, fwr, lon, lof):
    n = 4
    me = lax.axis_index("dp")
    right, left, opp = lax.rem(me + 1, n), lax.rem(me + 3, n), lax.rem(me + 2, n)
    sides = (right, left)
    rows = h1.shape[2]
    half = rows // 2
    odd = lax.rem(lax.axis_index("rep"), 2)
    groups = pieces // GROUP - odd * LATER
    chunk = a_buf.shape[1] // FIRST

    def rows_of(owner, h=None):
        start = owner * rows + (0 if h is None else h * half)
        return pl.ds(pl.multiple_of(start, 16), rows if h is None else half)

    def block(ref, p, width, owner, h=None):
        m, q = lax.div(p, per), lax.rem(p, per)
        return ref.at[m, rows_of(owner, h), pl.ds(pl.multiple_of(q * WIDTH, WIDTH), width)]

    def load_a(m):
        return pltpu.make_async_copy(a_ref.at[0, m], a_buf.at[lax.rem(m, 2)], a_sem.at[lax.rem(m, 2)])

    def load_g(p):
        m, q = lax.div(p, per), lax.rem(p, per)
        slot = lax.rem(p, 3)
        cols = pl.ds(pl.multiple_of(q * WIDTH, WIDTH), WIDTH)
        return pltpu.make_async_copy(g_ref.at[0, m, :, cols], g_buf.at[slot], g_sem.at[slot])

    def first(k):
        t = pl.ds(pl.multiple_of(k * chunk, chunk), chunk)
        return (
            pltpu.make_async_copy(g_ref.at[0, 0, t, pl.ds(0, WIDTH)], g_buf.at[0, t], f_sem.at[k, 0]),
            pltpu.make_async_copy(a_ref.at[0, 0, t], a_buf.at[0, t], f_sem.at[k, 1]),
        )

    def remote(src, dst, ss, rs, d):
        return pltpu.make_async_remote_copy(
            src_ref=src, dst_ref=dst, send_sem=ss, recv_sem=rs, device_id={"dp": sides[d]}, device_id_type=MESH
        )

    def send1(p, d):
        slot = lax.rem(p, SEND)
        return remote(sb1.at[slot, d], h1.at[p, d], s1s.at[slot, d], s1r.at[lax.rem(p, RECV), d], d)

    def send2(p, d):
        slot = lax.rem(p, SEND)
        return remote(sb2.at[slot, d], h2.at[p, d], s2s.at[slot, d], s2r.at[lax.rem(p, RECV), d], d)

    def load1(p, d):
        slot = lax.rem(p, V1)
        return pltpu.make_async_copy(h1.at[p, d], v1.at[slot, d], l1.at[lax.rem(p, 2), d])

    def load2(p, d):
        slot = lax.rem(p, V2)
        return pltpu.make_async_copy(h2.at[p, d], v2.at[slot, d], l2.at[lax.rem(p, 2), d])

    def gather(k, d):
        b = block(land, k * GROUP, GROUP * WIDTH, me)
        return remote(block(res, k * GROUP, GROUP * WIDTH, me), b, ags.at[lax.rem(k, KEEP), d], agr.at[k, d], d)

    def forward(k, d, to):
        p, width, owner = k * GROUP, GROUP * WIDTH, (left, right)[d]
        return remote(
            block(land, p, width, owner, d), block(to, p, width, owner, d), fws.at[lax.rem(k, KEEP), d], fwr.at[k, d], d
        )

    def keep_near(k, d):
        p, width, owner = k * GROUP, GROUP * WIDTH, (left, right)[d]
        return pltpu.make_async_copy(
            block(land, p, width, owner), block(res, p, width, owner), lon.at[lax.rem(k, KEEP), d]
        )

    def keep_far(k, d):
        p, width = k * GROUP, GROUP * WIDTH
        return pltpu.make_async_copy(
            block(land, p, width, opp, d), block(res, p, width, opp, d), lof.at[lax.rem(k, KEEP), d]
        )

    def gather_start(k):
        @pl.when(k >= KEEP)
        def _():
            for d in range(2):
                gather(k - KEEP, d).wait_send()

        for d in range(2):
            gather(k, d).start()

    def forward_start(k, to=land):
        @pl.when(k >= KEEP)
        def _():
            for d in range(2):
                forward(k - KEEP, d, land).wait_send()
                keep_near(k - KEEP, d).wait()

        for d in range(2):
            gather(k, d).wait_recv()
            forward(k, d, to).start()
            keep_near(k, d).start()

    def far_start(k):
        @pl.when(k >= KEEP)
        def _():
            for d in range(2):
                keep_far(k - KEEP, d).wait()

        for d in range(2):
            forward(k, d, land).wait_recv()
            keep_far(k, d).start()

    for k in range(FIRST):
        for copy in first(k):
            copy.start()
    load_g(1).start()

    barrier = pltpu.get_barrier_semaphore()
    for d in sides:
        pl.semaphore_signal(barrier, inc=1, device_id={"dp": d}, device_id_type=MESH)

    def product(lhs, rhs):
        return lax.dot_general(lhs, rhs, (((0,), (0,)), ((), ())), preferred_element_type=jnp.float32)

    acc[0] = jnp.zeros_like(acc[0])

    def first_step(k, carry):
        for copy in first(k):
            copy.wait()
        t = pl.ds(pl.multiple_of(k * chunk, chunk), chunk)
        acc[0] += product(a_buf[0, t], g_buf[0, t])
        return carry

    lax.fori_loop(0, FIRST, first_step, 0)
    pl.semaphore_wait(barrier, 2)

    def step(i, carry):
        @pl.when(i < pieces)
        def _():
            m, q = lax.div(i, per), lax.rem(i, per)
            slot, mine = lax.rem(i, SEND), lax.rem(i, ACC)

            @pl.when(i + 2 < pieces)
            def _():
                load_g(i + 2).start()

            @pl.when((q == 0) & (i + per < pieces))
            def _():
                load_a(m + 1).start()

            @pl.when(i > 0)
            def _():
                @pl.when(q == 0)
                def _():
                    load_a(m).wait()

                load_g(i).wait()
                acc[mine] = product(a_buf[lax.rem(m, 2)], g_buf[lax.rem(i, 3)])

            @pl.when(i >= SEND)
            def _():
                for d in range(2):
                    send1(i - SEND, d).wait_send()

            for d in range(2):
                sb1[slot, d, :half] = acc[mine, rows_of(opp, d)].astype(BF16)
                sb1[slot, d, half:] = acc[mine, rows_of(sides[d], 1 - d)].astype(BF16)
            for d in range(2):
                send1(i, d).start()

        @pl.when((i >= T1) & (i < pieces + T1))
        def _():
            for d in range(2):
                send1(i - T1, d).wait_recv()
                load1(i - T1, d).start()

        @pl.when((i >= T2) & (i < pieces + T2))
        def _():
            p = i - T2
            slot, mine, here = lax.rem(p, SEND), lax.rem(p, ACC), lax.rem(p, V1)

            @pl.when(p >= SEND)
            def _():
                for d in range(2):
                    send2(p - SEND, d).wait_send()

            for d in range(2):
                load1(p, d).wait()
                sb2[slot, d] = (acc[mine, rows_of(sides[d], d)] + v1[here, d, :half].astype(jnp.float32)).astype(BF16)
            for d in range(2):
                send2(p, d).start()

        @pl.when((i >= T3) & (i < pieces + T3))
        def _():
            for d in range(2):
                send2(i - T3, d).wait_recv()
                load2(i - T3, d).start()

        @pl.when(i >= T4)
        def _():
            p = i - T4
            m, q = lax.div(p, per), lax.rem(p, per)
            mine, one, two = lax.rem(p, ACC), lax.rem(p, V1), lax.rem(p, V2)
            cols = pl.ds(pl.multiple_of(q * WIDTH, WIDTH), WIDTH)
            for d in range(2):
                load2(p, d).wait()
                res[m, rows_of(me, d), cols] = (
                    acc[mine, rows_of(me, d)]
                    + v2[two, d].astype(jnp.float32)
                    + v1[one, 1 - d, half:].astype(jnp.float32)
                ).astype(BF16)

        t = i - OFFSET

        @pl.when((t >= 0) & (lax.rem(t, EVERY) == 0))
        def _():
            gather_start(lax.div(t, EVERY))

        @pl.when((t >= FWD) & (lax.rem(t - FWD, EVERY) == 0))
        def _():
            k = lax.div(t - FWD, EVERY)
            forward_start(k)

            @pl.when(k >= 2)
            def _():
                far_start(k - 2)

        return carry

    last = pieces + T4
    lax.fori_loop(0, last, step, 0)

    def over(f, start, stop):
        def body(k, carry):
            f(k)
            return carry

        lax.fori_loop(start, stop, body, 0)

    gathered = (last - 1 - OFFSET) // EVERY + 1
    forwarded = (last - 1 - OFFSET - FWD) // EVERY + 1
    kept = max(forwarded - 2, 0)
    final = groups - 1

    def tail(t):
        @pl.when((t >= gathered) & (t < groups))
        def _():
            gather_start(t)

        @pl.when((t - DEEP >= forwarded) & (t - DEEP < final))
        def _():
            forward_start(t - DEEP)

        @pl.when(t - DEEP == final)
        def _():
            forward_start(final, res)

        @pl.when((t - DEEP - 2 >= kept) & (t - DEEP - 2 < final))
        def _():
            far_start(t - DEEP - 2)

    over(tail, min(gathered, forwarded + DEEP, kept + DEEP + 2), groups + DEEP + 2)

    for p in range(pieces - SEND, pieces):
        for d in range(2):
            send1(p, d).wait_send()
            send2(p, d).wait_send()

    def drain(k):
        for d in range(2):
            gather(k, d).wait_send()
            keep_near(k, d).wait()
            forward(k, d, land).wait_send()

    def drain_far(k):
        for d in range(2):
            keep_far(k, d).wait()

    over(drain, groups - KEEP, groups)
    over(drain_far, final - KEEP, final)
    for d in range(2):
        forward(final, d, res).wait_recv()


def later_kernel(per, groups, res, after, land, sg, rg, sf, rf, sl):
    n = 4
    odd = lax.rem(lax.axis_index("rep"), 2)
    me = lax.axis_index("dp")
    right, left = lax.rem(me + 1, n), lax.rem(me + 3, n)
    sides = (right, left)
    rows = res.shape[1] // n
    half = rows // 2

    def rows_of(owner, h=0, size=rows):
        return pl.ds(pl.multiple_of(owner * rows + h * half, 16), size)

    def own(k):
        p = (groups - LATER + k) * GROUP
        return res.at[p // per, rows_of(me), pl.ds(p % per * WIDTH, GROUP * WIDTH)]

    def remote(src, dst, ss, rs, d):
        return pltpu.make_async_remote_copy(
            src_ref=src, dst_ref=dst, send_sem=ss, recv_sem=rs, device_id={"dp": sides[d]}, device_id_type=MESH
        )

    def gather(k, d):
        return remote(own(k), land.at[k, rows_of(me)], sg.at[k, d], rg.at[k, d], d)

    def forward(k, d):
        b = land.at[k, rows_of((left, right)[d], d, half)]
        return remote(b, b, sf.at[k, d], rf.at[k, d], d)

    def keep(k):
        return pltpu.make_async_copy(own(k), land.at[k, rows_of(me)], sl.at[k])

    @pl.when(odd == 1)
    def _():
        barrier = pltpu.get_barrier_semaphore()
        for d in sides:
            pl.semaphore_signal(barrier, inc=1, device_id={"dp": d}, device_id_type=MESH)
        pl.semaphore_wait(barrier, 2)
        every = [(k, d) for k in range(LATER) for d in range(2)]
        for k, d in every:
            gather(k, d).start()
        for k in range(LATER):
            keep(k).start()
        for k, d in every:
            gather(k, d).wait_recv()
            forward(k, d).start()
        for k in range(LATER):
            keep(k).wait()
        for k, d in every:
            gather(k, d).wait_send()
            forward(k, d).wait()


def write_kernel(per, begin, end_even, end_odd, res, *rest):
    o_ref, done, sem = rest[-3:]
    odd = lax.rem(lax.axis_index("rep"), 2)
    end = (1 - odd) * end_even + odd * end_odd

    def copy(k):
        p = k * GROUP
        to = o_ref.at[p // per, :, pl.ds(p % per * WIDTH, GROUP * WIDTH)]
        part = res.at[k - begin] if begin else res.at[p // per, :, pl.ds(p % per * WIDTH, GROUP * WIDTH)]
        return pltpu.make_async_copy(part, to, sem.at[k])

    for k in range(begin, max(end_even, end_odd)):
        @pl.when(k < end)
        def _():
            copy(k).start()

    for k in range(begin, max(end_even, end_odd)):
        @pl.when(k < end)
        def _():
            copy(k).wait()


def solution(mesh):
    def local(a, g):
        _, count, tokens, d = a.shape
        ff = g.shape[3]
        per = ff // WIDTH
        pieces = count * per
        rows = d // mesh.shape["dp"]
        groups = pieces // GROUP
        dma = pltpu.SemaphoreType.DMA
        vmem = pl.BlockSpec(memory_space=pltpu.VMEM)
        hbm = pl.BlockSpec(memory_space=pltpu.HBM)
        token = jax.ShapeDtypeStruct((8, 128), BF16)
        res = pl.pallas_call(
            functools.partial(sums_kernel, per, pieces),
            out_shape=(
                pltpu.VMEM((count, d, ff), BF16),
                jax.ShapeDtypeStruct((count, d, ff), BF16),
                jax.ShapeDtypeStruct((pieces, 2, rows, WIDTH), BF16),
                jax.ShapeDtypeStruct((pieces, 2, rows // 2, WIDTH), BF16),
            ),
            in_specs=[hbm] * 2,
            out_specs=(vmem, hbm, hbm, hbm),
            scratch_shapes=[
                pltpu.VMEM((2, tokens, d), BF16),
                pltpu.VMEM((3, tokens, WIDTH), BF16),
                pltpu.VMEM((ACC, d, WIDTH), jnp.float32),
                pltpu.VMEM((SEND, 2, rows, WIDTH), BF16),
                pltpu.VMEM((SEND, 2, rows // 2, WIDTH), BF16),
                pltpu.VMEM((V1, 2, rows, WIDTH), BF16),
                pltpu.VMEM((V2, 2, rows // 2, WIDTH), BF16),
                dma((2,)),
                dma((3,)),
                dma((FIRST, 2)),
                dma((SEND, 2)),
                dma((RECV, 2)),
                dma((SEND, 2)),
                dma((RECV, 2)),
                dma((2, 2)),
                dma((2, 2)),
                dma((KEEP, 2)),
                dma((groups, 2)),
                dma((KEEP, 2)),
                dma((groups, 2)),
                dma((KEEP, 2)),
                dma((KEEP, 2)),
            ],
            compiler_params=pltpu.CompilerParams(
                collective_id=0, has_side_effects=True, vmem_limit_bytes=40 * 1024 * 1024
            ),
            name="sums",
        )(a, g)[0]

        def write(begin, end_even, end_odd, *args):
            return pl.pallas_call(
                functools.partial(write_kernel, per, begin, end_even, end_odd),
                out_shape=(jax.ShapeDtypeStruct((count, d, ff), BF16), token),
                in_specs=[vmem, hbm][: len(args)],
                out_specs=(hbm, hbm),
                input_output_aliases={1: 0} if begin else {},
                scratch_shapes=[dma((groups,))],
                compiler_params=pltpu.CompilerParams(vmem_limit_bytes=4 * 1024 * 1024),
                name=f"write{begin}",
            )(*args)

        split = groups - LATER
        out, done = write(0, groups, split, res)
        later = pl.pallas_call(
            functools.partial(later_kernel, per, groups),
            out_shape=pltpu.VMEM((LATER, d, GROUP * WIDTH), BF16),
            in_specs=[vmem, hbm],
            out_specs=vmem,
            scratch_shapes=[dma((LATER, 2))] * 4 + [dma((LATER,))],
            compiler_params=pltpu.CompilerParams(
                collective_id=1, has_side_effects=True, vmem_limit_bytes=4 * 1024 * 1024
            ),
            name="later",
        )(res, done)
        return write(split, split, groups, later, out)[0]

    return jax.shard_map(
        local,
        mesh=mesh,
        in_specs=(P(("rep", "dp")), P(("rep", "dp"))),
        out_specs=P("rep"),
        check_vma=False,
    )
```

```python
import functools

import jax
import jax.numpy as jnp
from jax import lax
from jax.experimental import pallas as pl
from jax.experimental.pallas import tpu as pltpu
from jax.sharding import PartitionSpec as P

MESH = pl.DeviceIdType.MESH
BF16 = jnp.bfloat16
WIDTH = 256
GROUP = 3
FIRST = 4
T1, T2, T3, T4 = 3, 4, 6, 7
EVERY, OFFSET = 4, 9
LATER = 2
DEEP = 3
FWD = 2
ACC, V1, V2, SEND = T4 + 1, T4 - T1 + 1, T4 - T3 + 1, 4
RECV, KEEP = 7, 4


def sums_kernel(per, pieces, a_ref, g_ref, res, land, h1, h2, a_buf, g_buf, acc, sb1, sb2, v1, v2,
                a_sem, g_sem, f_sem, s1s, s1r, s2s, s2r, l1, l2, ags, agr, fws, fwr, lon, lof):
    n = 4
    me = lax.axis_index("dp")
    right, left, opp = lax.rem(me + 1, n), lax.rem(me + 3, n), lax.rem(me + 2, n)
    sides = (right, left)
    rows = h1.shape[2]
    half = rows // 2
    odd = lax.rem(lax.axis_index("rep"), 2)
    groups = pieces // GROUP - odd * LATER
    chunk = a_buf.shape[1] // FIRST

    def rows_of(owner, h=None):
        start = owner * rows + (0 if h is None else h * half)
        return pl.ds(pl.multiple_of(start, 16), rows if h is None else half)

    def block(ref, p, width, owner, h=None):
        m, q = lax.div(p, per), lax.rem(p, per)
        return ref.at[m, rows_of(owner, h), pl.ds(pl.multiple_of(q * WIDTH, WIDTH), width)]

    def load_a(m):
        return pltpu.make_async_copy(a_ref.at[0, m], a_buf.at[lax.rem(m, 2)], a_sem.at[lax.rem(m, 2)])

    def load_g(p):
        m, q = lax.div(p, per), lax.rem(p, per)
        slot = lax.rem(p, 3)
        cols = pl.ds(pl.multiple_of(q * WIDTH, WIDTH), WIDTH)
        return pltpu.make_async_copy(g_ref.at[0, m, :, cols], g_buf.at[slot], g_sem.at[slot])

    def first(k):
        t = pl.ds(pl.multiple_of(k * chunk, chunk), chunk)
        return (
            pltpu.make_async_copy(g_ref.at[0, 0, t, pl.ds(0, WIDTH)], g_buf.at[0, t], f_sem.at[k, 0]),
            pltpu.make_async_copy(a_ref.at[0, 0, t], a_buf.at[0, t], f_sem.at[k, 1]),
        )

    def remote(src, dst, ss, rs, d):
        return pltpu.make_async_remote_copy(
            src_ref=src, dst_ref=dst, send_sem=ss, recv_sem=rs, device_id={"dp": sides[d]}, device_id_type=MESH
        )

    def send1(p, d):
        slot = lax.rem(p, SEND)
        return remote(sb1.at[slot, d], h1.at[p, d], s1s.at[slot, d], s1r.at[lax.rem(p, RECV), d], d)

    def send2(p, d):
        slot = lax.rem(p, SEND)
        return remote(sb2.at[slot, d], h2.at[p, d], s2s.at[slot, d], s2r.at[lax.rem(p, RECV), d], d)

    def load1(p, d):
        slot = lax.rem(p, V1)
        return pltpu.make_async_copy(h1.at[p, d], v1.at[slot, d], l1.at[lax.rem(p, 2), d])

    def load2(p, d):
        slot = lax.rem(p, V2)
        return pltpu.make_async_copy(h2.at[p, d], v2.at[slot, d], l2.at[lax.rem(p, 2), d])

    def gather(k, d):
        b = block(land, k * GROUP, GROUP * WIDTH, me)
        return remote(block(res, k * GROUP, GROUP * WIDTH, me), b, ags.at[lax.rem(k, KEEP), d], agr.at[k, d], d)

    def forward(k, d, to):
        p, width, owner = k * GROUP, GROUP * WIDTH, (left, right)[d]
        return remote(
            block(land, p, width, owner, d), block(to, p, width, owner, d), fws.at[lax.rem(k, KEEP), d], fwr.at[k, d], d
        )

    def keep_near(k, d):
        p, width, owner = k * GROUP, GROUP * WIDTH, (left, right)[d]
        return pltpu.make_async_copy(
            block(land, p, width, owner), block(res, p, width, owner), lon.at[lax.rem(k, KEEP), d]
        )

    def keep_far(k, d):
        p, width = k * GROUP, GROUP * WIDTH
        return pltpu.make_async_copy(
            block(land, p, width, opp, d), block(res, p, width, opp, d), lof.at[lax.rem(k, KEEP), d]
        )

    def gather_start(k):
        @pl.when(k >= KEEP)
        def _():
            for d in range(2):
                gather(k - KEEP, d).wait_send()

        for d in range(2):
            gather(k, d).start()

    def forward_start(k, to=land):
        @pl.when(k >= KEEP)
        def _():
            for d in range(2):
                forward(k - KEEP, d, land).wait_send()
                keep_near(k - KEEP, d).wait()

        for d in range(2):
            gather(k, d).wait_recv()
            forward(k, d, to).start()
            keep_near(k, d).start()

    def far_start(k):
        @pl.when(k >= KEEP)
        def _():
            for d in range(2):
                keep_far(k - KEEP, d).wait()

        for d in range(2):
            forward(k, d, land).wait_recv()
            keep_far(k, d).start()

    for k in range(FIRST):
        for copy in first(k):
            copy.start()
    load_g(1).start()

    barrier = pltpu.get_barrier_semaphore()
    for d in sides:
        pl.semaphore_signal(barrier, inc=1, device_id={"dp": d}, device_id_type=MESH)

    def product(lhs, rhs):
        return lax.dot_general(lhs, rhs, (((0,), (0,)), ((), ())), preferred_element_type=jnp.float32)

    acc[0] = jnp.zeros_like(acc[0])

    def first_step(k, carry):
        for copy in first(k):
            copy.wait()
        t = pl.ds(pl.multiple_of(k * chunk, chunk), chunk)
        acc[0] += product(a_buf[0, t], g_buf[0, t])
        return carry

    lax.fori_loop(0, FIRST, first_step, 0)
    pl.semaphore_wait(barrier, 2)

    def step(i, carry):
        @pl.when(i < pieces)
        def _():
            m, q = lax.div(i, per), lax.rem(i, per)
            slot, mine = lax.rem(i, SEND), lax.rem(i, ACC)

            @pl.when(i + 2 < pieces)
            def _():
                load_g(i + 2).start()

            @pl.when((q == 0) & (i + per < pieces))
            def _():
                load_a(m + 1).start()

            @pl.when(i > 0)
            def _():
                @pl.when(q == 0)
                def _():
                    load_a(m).wait()

                load_g(i).wait()
                acc[mine] = product(a_buf[lax.rem(m, 2)], g_buf[lax.rem(i, 3)])

            @pl.when(i >= SEND)
            def _():
                for d in range(2):
                    send1(i - SEND, d).wait_send()

            for d in range(2):
                sb1[slot, d, :half] = acc[mine, rows_of(opp, d)].astype(BF16)
                sb1[slot, d, half:] = acc[mine, rows_of(sides[d], 1 - d)].astype(BF16)
            for d in range(2):
                send1(i, d).start()

        @pl.when((i >= T1) & (i < pieces + T1))
        def _():
            for d in range(2):
                send1(i - T1, d).wait_recv()
                load1(i - T1, d).start()

        @pl.when((i >= T2) & (i < pieces + T2))
        def _():
            p = i - T2
            slot, mine, here = lax.rem(p, SEND), lax.rem(p, ACC), lax.rem(p, V1)

            @pl.when(p >= SEND)
            def _():
                for d in range(2):
                    send2(p - SEND, d).wait_send()

            for d in range(2):
                load1(p, d).wait()
                sb2[slot, d] = (acc[mine, rows_of(sides[d], d)] + v1[here, d, :half].astype(jnp.float32)).astype(BF16)
            for d in range(2):
                send2(p, d).start()

        @pl.when((i >= T3) & (i < pieces + T3))
        def _():
            for d in range(2):
                send2(i - T3, d).wait_recv()
                load2(i - T3, d).start()

        @pl.when(i >= T4)
        def _():
            p = i - T4
            m, q = lax.div(p, per), lax.rem(p, per)
            mine, one, two = lax.rem(p, ACC), lax.rem(p, V1), lax.rem(p, V2)
            cols = pl.ds(pl.multiple_of(q * WIDTH, WIDTH), WIDTH)
            for d in range(2):
                load2(p, d).wait()
                res[m, rows_of(me, d), cols] = (
                    acc[mine, rows_of(me, d)]
                    + v2[two, d].astype(jnp.float32)
                    + v1[one, 1 - d, half:].astype(jnp.float32)
                ).astype(BF16)

        t = i - OFFSET

        @pl.when((t >= 0) & (lax.rem(t, EVERY) == 0))
        def _():
            gather_start(lax.div(t, EVERY))

        @pl.when((t >= FWD) & (lax.rem(t - FWD, EVERY) == 0))
        def _():
            k = lax.div(t - FWD, EVERY)
            forward_start(k)

            @pl.when(k >= 2)
            def _():
                far_start(k - 2)

        return carry

    last = pieces + T4
    lax.fori_loop(0, last, step, 0)

    def over(f, start, stop):
        def body(k, carry):
            f(k)
            return carry

        lax.fori_loop(start, stop, body, 0)

    gathered = (last - 1 - OFFSET) // EVERY + 1
    forwarded = (last - 1 - OFFSET - FWD) // EVERY + 1
    kept = max(forwarded - 2, 0)
    final = groups - 1

    def tail(t):
        @pl.when((t >= gathered) & (t < groups))
        def _():
            gather_start(t)

        @pl.when((t - DEEP >= forwarded) & (t - DEEP < final))
        def _():
            forward_start(t - DEEP)

        @pl.when(t - DEEP == final)
        def _():
            forward_start(final, res)

        @pl.when((t - DEEP - 2 >= kept) & (t - DEEP - 2 < final))
        def _():
            far_start(t - DEEP - 2)

    over(tail, min(gathered, forwarded + DEEP, kept + DEEP + 2), groups + DEEP + 2)

    for p in range(pieces - SEND, pieces):
        for d in range(2):
            send1(p, d).wait_send()
            send2(p, d).wait_send()

    def drain(k):
        for d in range(2):
            gather(k, d).wait_send()
            keep_near(k, d).wait()
            forward(k, d, land).wait_send()

    def drain_far(k):
        for d in range(2):
            keep_far(k, d).wait()

    over(drain, groups - KEEP, groups)
    over(drain_far, final - KEEP, final)
    for d in range(2):
        forward(final, d, res).wait_recv()


def later_kernel(per, groups, res, after, land, sg, rg, sf, rf, sl):
    n = 4
    odd = lax.rem(lax.axis_index("rep"), 2)
    me = lax.axis_index("dp")
    right, left = lax.rem(me + 1, n), lax.rem(me + 3, n)
    sides = (right, left)
    rows = res.shape[1] // n
    half = rows // 2

    def rows_of(owner, h=0, size=rows):
        return pl.ds(pl.multiple_of(owner * rows + h * half, 16), size)

    def own(k):
        p = (groups - LATER + k) * GROUP
        return res.at[p // per, rows_of(me), pl.ds(p % per * WIDTH, GROUP * WIDTH)]

    def remote(src, dst, ss, rs, d):
        return pltpu.make_async_remote_copy(
            src_ref=src, dst_ref=dst, send_sem=ss, recv_sem=rs, device_id={"dp": sides[d]}, device_id_type=MESH
        )

    def gather(k, d):
        return remote(own(k), land.at[k, rows_of(me)], sg.at[k, d], rg.at[k, d], d)

    def forward(k, d):
        b = land.at[k, rows_of((left, right)[d], d, half)]
        return remote(b, b, sf.at[k, d], rf.at[k, d], d)

    def keep(k):
        return pltpu.make_async_copy(own(k), land.at[k, rows_of(me)], sl.at[k])

    @pl.when(odd == 1)
    def _():
        barrier = pltpu.get_barrier_semaphore()
        for d in sides:
            pl.semaphore_signal(barrier, inc=1, device_id={"dp": d}, device_id_type=MESH)
        pl.semaphore_wait(barrier, 2)
        every = [(k, d) for k in range(LATER) for d in range(2)]
        for k, d in every:
            gather(k, d).start()
        for k in range(LATER):
            keep(k).start()
        for k, d in every:
            gather(k, d).wait_recv()
            forward(k, d).start()
        for k in range(LATER):
            keep(k).wait()
        for k, d in every:
            gather(k, d).wait_send()
            forward(k, d).wait()


def write_kernel(per, begin, end_even, end_odd, res, *rest):
    o_ref, done, sem = rest[-3:]
    odd = lax.rem(lax.axis_index("rep"), 2)
    end = (1 - odd) * end_even + odd * end_odd

    def copy(k):
        p = k * GROUP
        to = o_ref.at[p // per, :, pl.ds(p % per * WIDTH, GROUP * WIDTH)]
        part = res.at[k - begin] if begin else res.at[p // per, :, pl.ds(p % per * WIDTH, GROUP * WIDTH)]
        return pltpu.make_async_copy(part, to, sem.at[k])

    for k in range(begin, max(end_even, end_odd)):
        @pl.when(k < end)
        def _():
            copy(k).start()

    for k in range(begin, max(end_even, end_odd)):
        @pl.when(k < end)
        def _():
            copy(k).wait()


def solution(mesh):
    def local(a, g):
        _, count, tokens, d = a.shape
        ff = g.shape[3]
        per = ff // WIDTH
        pieces = count * per
        rows = d // mesh.shape["dp"]
        groups = pieces // GROUP
        dma = pltpu.SemaphoreType.DMA
        vmem = pl.BlockSpec(memory_space=pltpu.VMEM)
        hbm = pl.BlockSpec(memory_space=pltpu.HBM)
        token = jax.ShapeDtypeStruct((8, 128), BF16)
        res = pl.pallas_call(
            functools.partial(sums_kernel, per, pieces),
            out_shape=(
                pltpu.VMEM((count, d, ff), BF16),
                jax.ShapeDtypeStruct((count, d, ff), BF16),
                jax.ShapeDtypeStruct((pieces, 2, rows, WIDTH), BF16),
                jax.ShapeDtypeStruct((pieces, 2, rows // 2, WIDTH), BF16),
            ),
            in_specs=[hbm] * 2,
            out_specs=(vmem, hbm, hbm, hbm),
            scratch_shapes=[
                pltpu.VMEM((2, tokens, d), BF16),
                pltpu.VMEM((3, tokens, WIDTH), BF16),
                pltpu.VMEM((ACC, d, WIDTH), jnp.float32),
                pltpu.VMEM((SEND, 2, rows, WIDTH), BF16),
                pltpu.VMEM((SEND, 2, rows // 2, WIDTH), BF16),
                pltpu.VMEM((V1, 2, rows, WIDTH), BF16),
                pltpu.VMEM((V2, 2, rows // 2, WIDTH), BF16),
                dma((2,)),
                dma((3,)),
                dma((FIRST, 2)),
                dma((SEND, 2)),
                dma((RECV, 2)),
                dma((SEND, 2)),
                dma((RECV, 2)),
                dma((2, 2)),
                dma((2, 2)),
                dma((KEEP, 2)),
                dma((groups, 2)),
                dma((KEEP, 2)),
                dma((groups, 2)),
                dma((KEEP, 2)),
                dma((KEEP, 2)),
            ],
            compiler_params=pltpu.CompilerParams(
                collective_id=0, has_side_effects=True, vmem_limit_bytes=40 * 1024 * 1024
            ),
            name="sums",
        )(a, g)[0]

        def write(begin, end_even, end_odd, *args):
            return pl.pallas_call(
                functools.partial(write_kernel, per, begin, end_even, end_odd),
                out_shape=(jax.ShapeDtypeStruct((count, d, ff), BF16), token),
                in_specs=[vmem, hbm][: len(args)],
                out_specs=(hbm, hbm),
                input_output_aliases={1: 0} if begin else {},
                scratch_shapes=[dma((groups,))],
                compiler_params=pltpu.CompilerParams(vmem_limit_bytes=4 * 1024 * 1024),
                name=f"write{begin}",
            )(*args)

        split = groups - LATER
        out, done = write(0, groups, split, res)
        later = pl.pallas_call(
            functools.partial(later_kernel, per, groups),
            out_shape=pltpu.VMEM((LATER, d, GROUP * WIDTH), BF16),
            in_specs=[vmem, hbm],
            out_specs=vmem,
            scratch_shapes=[dma((LATER, 2))] * 4 + [dma((LATER,))],
            compiler_params=pltpu.CompilerParams(
                collective_id=1, has_side_effects=True, vmem_limit_bytes=4 * 1024 * 1024
            ),
            name="later",
        )(res, done)
        return write(split, split, groups, later, out)[0]

    return jax.shard_map(
        local,
        mesh=mesh,
        in_specs=(P(("rep", "dp")), P(("rep", "dp"))),
        out_specs=P("rep"),
        check_vma=False,
    )
```

```python
import functools

import jax
import jax.numpy as jnp
from jax import lax
from jax.experimental import pallas as pl
from jax.experimental.pallas import tpu as pltpu
from jax.sharding import PartitionSpec as P

MESH = pl.DeviceIdType.MESH
BF16 = jnp.bfloat16
WIDTH = 256
GROUP = 3
FIRST = 4
T1, T2, T3, T4 = 3, 4, 6, 7
EVERY, OFFSET = 4, 9
LATER = 2
DEEP = 3
FWD = 2
ACC, V1, V2, SEND = T4 + 1, T4 - T1 + 1, T4 - T3 + 1, 4
RECV, KEEP = 7, 4


def sums_kernel(per, pieces, a_ref, g_ref, res, land, h1, h2, a_buf, g_buf, acc, sb1, sb2, v1, v2,
                a_sem, g_sem, f_sem, s1s, s1r, s2s, s2r, l1, l2, ags, agr, fws, fwr, lon, lof):
    n = 4
    me = lax.axis_index("dp")
    right, left, opp = lax.rem(me + 1, n), lax.rem(me + 3, n), lax.rem(me + 2, n)
    sides = (right, left)
    rows = h1.shape[2]
    half = rows // 2
    odd = lax.rem(lax.axis_index("rep"), 2)
    groups = pieces // GROUP - odd * LATER
    chunk = a_buf.shape[1] // FIRST

    def rows_of(owner, h=None):
        start = owner * rows + (0 if h is None else h * half)
        return pl.ds(pl.multiple_of(start, 16), rows if h is None else half)

    def block(ref, p, width, owner, h=None):
        m, q = lax.div(p, per), lax.rem(p, per)
        return ref.at[m, rows_of(owner, h), pl.ds(pl.multiple_of(q * WIDTH, WIDTH), width)]

    def load_a(m):
        return pltpu.make_async_copy(a_ref.at[0, m], a_buf.at[lax.rem(m, 2)], a_sem.at[lax.rem(m, 2)])

    def load_g(p):
        m, q = lax.div(p, per), lax.rem(p, per)
        slot = lax.rem(p, 3)
        cols = pl.ds(pl.multiple_of(q * WIDTH, WIDTH), WIDTH)
        return pltpu.make_async_copy(g_ref.at[0, m, :, cols], g_buf.at[slot], g_sem.at[slot])

    def first(k):
        t = pl.ds(pl.multiple_of(k * chunk, chunk), chunk)
        return (
            pltpu.make_async_copy(g_ref.at[0, 0, t, pl.ds(0, WIDTH)], g_buf.at[0, t], f_sem.at[k, 0]),
            pltpu.make_async_copy(a_ref.at[0, 0, t], a_buf.at[0, t], f_sem.at[k, 1]),
        )

    def remote(src, dst, ss, rs, d):
        return pltpu.make_async_remote_copy(
            src_ref=src, dst_ref=dst, send_sem=ss, recv_sem=rs, device_id={"dp": sides[d]}, device_id_type=MESH
        )

    def send1(p, d):
        slot = lax.rem(p, SEND)
        return remote(sb1.at[slot, d], h1.at[p, d], s1s.at[slot, d], s1r.at[lax.rem(p, RECV), d], d)

    def send2(p, d):
        slot = lax.rem(p, SEND)
        return remote(sb2.at[slot, d], h2.at[p, d], s2s.at[slot, d], s2r.at[lax.rem(p, RECV), d], d)

    def load1(p, d):
        slot = lax.rem(p, V1)
        return pltpu.make_async_copy(h1.at[p, d], v1.at[slot, d], l1.at[lax.rem(p, 2), d])

    def load2(p, d):
        slot = lax.rem(p, V2)
        return pltpu.make_async_copy(h2.at[p, d], v2.at[slot, d], l2.at[lax.rem(p, 2), d])

    def gather(k, d):
        b = block(land, k * GROUP, GROUP * WIDTH, me)
        return remote(block(res, k * GROUP, GROUP * WIDTH, me), b, ags.at[lax.rem(k, KEEP), d], agr.at[k, d], d)

    def forward(k, d, to):
        p, width, owner = k * GROUP, GROUP * WIDTH, (left, right)[d]
        return remote(
            block(land, p, width, owner, d), block(to, p, width, owner, d), fws.at[lax.rem(k, KEEP), d], fwr.at[k, d], d
        )

    def keep_near(k, d):
        p, width, owner = k * GROUP, GROUP * WIDTH, (left, right)[d]
        return pltpu.make_async_copy(
            block(land, p, width, owner), block(res, p, width, owner), lon.at[lax.rem(k, KEEP), d]
        )

    def keep_far(k, d):
        p, width = k * GROUP, GROUP * WIDTH
        return pltpu.make_async_copy(
            block(land, p, width, opp, d), block(res, p, width, opp, d), lof.at[lax.rem(k, KEEP), d]
        )

    def gather_start(k):
        @pl.when(k >= KEEP)
        def _():
            for d in range(2):
                gather(k - KEEP, d).wait_send()

        for d in range(2):
            gather(k, d).start()

    def forward_start(k, to=land):
        @pl.when(k >= KEEP)
        def _():
            for d in range(2):
                forward(k - KEEP, d, land).wait_send()
                keep_near(k - KEEP, d).wait()

        for d in range(2):
            gather(k, d).wait_recv()
            forward(k, d, to).start()
            keep_near(k, d).start()

    def far_start(k):
        @pl.when(k >= KEEP)
        def _():
            for d in range(2):
                keep_far(k - KEEP, d).wait()

        for d in range(2):
            forward(k, d, land).wait_recv()
            keep_far(k, d).start()

    for k in range(FIRST):
        for copy in first(k)[::-1]:
            copy.start()
    load_g(1).start()

    barrier = pltpu.get_barrier_semaphore()
    for d in sides:
        pl.semaphore_signal(barrier, inc=1, device_id={"dp": d}, device_id_type=MESH)

    def product(lhs, rhs):
        return lax.dot_general(lhs, rhs, (((0,), (0,)), ((), ())), preferred_element_type=jnp.float32)

    acc[0] = jnp.zeros_like(acc[0])

    def first_step(k, carry):
        for copy in first(k):
            copy.wait()
        t = pl.ds(pl.multiple_of(k * chunk, chunk), chunk)
        acc[0] += product(a_buf[0, t], g_buf[0, t])
        return carry

    lax.fori_loop(0, FIRST, first_step, 0)
    pl.semaphore_wait(barrier, 2)

    def step(i, carry):
        @pl.when(i < pieces)
        def _():
            m, q = lax.div(i, per), lax.rem(i, per)
            slot, mine = lax.rem(i, SEND), lax.rem(i, ACC)

            @pl.when(i + 2 < pieces)
            def _():
                load_g(i + 2).start()

            @pl.when((q == 0) & (i + per < pieces))
            def _():
                load_a(m + 1).start()

            @pl.when(i > 0)
            def _():
                @pl.when(q == 0)
                def _():
                    load_a(m).wait()

                load_g(i).wait()
                acc[mine] = product(a_buf[lax.rem(m, 2)], g_buf[lax.rem(i, 3)])

            @pl.when(i >= SEND)
            def _():
                for d in range(2):
                    send1(i - SEND, d).wait_send()

            for d in range(2):
                sb1[slot, d, :half] = acc[mine, rows_of(opp, d)].astype(BF16)
                sb1[slot, d, half:] = acc[mine, rows_of(sides[d], 1 - d)].astype(BF16)
            for d in range(2):
                send1(i, d).start()

        @pl.when((i >= T1) & (i < pieces + T1))
        def _():
            for d in range(2):
                send1(i - T1, d).wait_recv()
                load1(i - T1, d).start()

        @pl.when((i >= T2) & (i < pieces + T2))
        def _():
            p = i - T2
            slot, mine, here = lax.rem(p, SEND), lax.rem(p, ACC), lax.rem(p, V1)

            @pl.when(p >= SEND)
            def _():
                for d in range(2):
                    send2(p - SEND, d).wait_send()

            for d in range(2):
                load1(p, d).wait()
                sb2[slot, d] = (acc[mine, rows_of(sides[d], d)] + v1[here, d, :half].astype(jnp.float32)).astype(BF16)
            for d in range(2):
                send2(p, d).start()

        @pl.when((i >= T3) & (i < pieces + T3))
        def _():
            for d in range(2):
                send2(i - T3, d).wait_recv()
                load2(i - T3, d).start()

        @pl.when(i >= T4)
        def _():
            p = i - T4
            m, q = lax.div(p, per), lax.rem(p, per)
            mine, one, two = lax.rem(p, ACC), lax.rem(p, V1), lax.rem(p, V2)
            cols = pl.ds(pl.multiple_of(q * WIDTH, WIDTH), WIDTH)
            for d in range(2):
                load2(p, d).wait()
                res[m, rows_of(me, d), cols] = (
                    acc[mine, rows_of(me, d)]
                    + v2[two, d].astype(jnp.float32)
                    + v1[one, 1 - d, half:].astype(jnp.float32)
                ).astype(BF16)

        t = i - OFFSET

        @pl.when((t >= 0) & (lax.rem(t, EVERY) == 0))
        def _():
            gather_start(lax.div(t, EVERY))

        @pl.when((t >= FWD) & (lax.rem(t - FWD, EVERY) == 0))
        def _():
            k = lax.div(t - FWD, EVERY)
            forward_start(k)

            @pl.when(k >= 2)
            def _():
                far_start(k - 2)

        return carry

    last = pieces + T4
    lax.fori_loop(0, last, step, 0)

    def over(f, start, stop):
        def body(k, carry):
            f(k)
            return carry

        lax.fori_loop(start, stop, body, 0)

    gathered = (last - 1 - OFFSET) // EVERY + 1
    forwarded = (last - 1 - OFFSET - FWD) // EVERY + 1
    kept = max(forwarded - 2, 0)
    final = groups - 1

    def tail(t):
        @pl.when((t >= gathered) & (t < groups))
        def _():
            gather_start(t)

        @pl.when((t - DEEP >= forwarded) & (t - DEEP < final))
        def _():
            forward_start(t - DEEP)

        @pl.when(t - DEEP == final)
        def _():
            forward_start(final, res)

        @pl.when((t - DEEP - 2 >= kept) & (t - DEEP - 2 < final))
        def _():
            far_start(t - DEEP - 2)

    over(tail, min(gathered, forwarded + DEEP, kept + DEEP + 2), groups + DEEP + 2)

    for p in range(pieces - SEND, pieces):
        for d in range(2):
            send1(p, d).wait_send()
            send2(p, d).wait_send()

    def drain(k):
        for d in range(2):
            gather(k, d).wait_send()
            keep_near(k, d).wait()
            forward(k, d, land).wait_send()

    def drain_far(k):
        for d in range(2):
            keep_far(k, d).wait()

    over(drain, groups - KEEP, groups)
    over(drain_far, final - KEEP, final)
    for d in range(2):
        forward(final, d, res).wait_recv()


def later_kernel(per, groups, res, after, land, sg, rg, sf, rf, sl):
    n = 4
    odd = lax.rem(lax.axis_index("rep"), 2)
    me = lax.axis_index("dp")
    right, left = lax.rem(me + 1, n), lax.rem(me + 3, n)
    sides = (right, left)
    rows = res.shape[1] // n
    half = rows // 2

    def rows_of(owner, h=0, size=rows):
        return pl.ds(pl.multiple_of(owner * rows + h * half, 16), size)

    def own(k):
        p = (groups - LATER + k) * GROUP
        return res.at[p // per, rows_of(me), pl.ds(p % per * WIDTH, GROUP * WIDTH)]

    def remote(src, dst, ss, rs, d):
        return pltpu.make_async_remote_copy(
            src_ref=src, dst_ref=dst, send_sem=ss, recv_sem=rs, device_id={"dp": sides[d]}, device_id_type=MESH
        )

    def gather(k, d):
        return remote(own(k), land.at[k, rows_of(me)], sg.at[k, d], rg.at[k, d], d)

    def forward(k, d):
        b = land.at[k, rows_of((left, right)[d], d, half)]
        return remote(b, b, sf.at[k, d], rf.at[k, d], d)

    def keep(k):
        return pltpu.make_async_copy(own(k), land.at[k, rows_of(me)], sl.at[k])

    @pl.when(odd == 1)
    def _():
        barrier = pltpu.get_barrier_semaphore()
        for d in sides:
            pl.semaphore_signal(barrier, inc=1, device_id={"dp": d}, device_id_type=MESH)
        pl.semaphore_wait(barrier, 2)
        every = [(k, d) for k in range(LATER) for d in range(2)]
        for k, d in every:
            gather(k, d).start()
        for k in range(LATER):
            keep(k).start()
        for k, d in every:
            gather(k, d).wait_recv()
            forward(k, d).start()
        for k in range(LATER):
            keep(k).wait()
        for k, d in every:
            gather(k, d).wait_send()
            forward(k, d).wait()


def write_kernel(per, begin, end_even, end_odd, res, *rest):
    o_ref, done, sem = rest[-3:]
    odd = lax.rem(lax.axis_index("rep"), 2)
    end = (1 - odd) * end_even + odd * end_odd

    def copy(k):
        p = k * GROUP
        to = o_ref.at[p // per, :, pl.ds(p % per * WIDTH, GROUP * WIDTH)]
        part = res.at[k - begin] if begin else res.at[p // per, :, pl.ds(p % per * WIDTH, GROUP * WIDTH)]
        return pltpu.make_async_copy(part, to, sem.at[k])

    for k in range(begin, max(end_even, end_odd)):
        @pl.when(k < end)
        def _():
            copy(k).start()

    for k in range(begin, max(end_even, end_odd)):
        @pl.when(k < end)
        def _():
            copy(k).wait()


def solution(mesh):
    def local(a, g):
        _, count, tokens, d = a.shape
        ff = g.shape[3]
        per = ff // WIDTH
        pieces = count * per
        rows = d // mesh.shape["dp"]
        groups = pieces // GROUP
        dma = pltpu.SemaphoreType.DMA
        vmem = pl.BlockSpec(memory_space=pltpu.VMEM)
        hbm = pl.BlockSpec(memory_space=pltpu.HBM)
        token = jax.ShapeDtypeStruct((8, 128), BF16)
        res = pl.pallas_call(
            functools.partial(sums_kernel, per, pieces),
            out_shape=(
                pltpu.VMEM((count, d, ff), BF16),
                jax.ShapeDtypeStruct((count, d, ff), BF16),
                jax.ShapeDtypeStruct((pieces, 2, rows, WIDTH), BF16),
                jax.ShapeDtypeStruct((pieces, 2, rows // 2, WIDTH), BF16),
            ),
            in_specs=[hbm] * 2,
            out_specs=(vmem, hbm, hbm, hbm),
            scratch_shapes=[
                pltpu.VMEM((2, tokens, d), BF16),
                pltpu.VMEM((3, tokens, WIDTH), BF16),
                pltpu.VMEM((ACC, d, WIDTH), jnp.float32),
                pltpu.VMEM((SEND, 2, rows, WIDTH), BF16),
                pltpu.VMEM((SEND, 2, rows // 2, WIDTH), BF16),
                pltpu.VMEM((V1, 2, rows, WIDTH), BF16),
                pltpu.VMEM((V2, 2, rows // 2, WIDTH), BF16),
                dma((2,)),
                dma((3,)),
                dma((FIRST, 2)),
                dma((SEND, 2)),
                dma((RECV, 2)),
                dma((SEND, 2)),
                dma((RECV, 2)),
                dma((2, 2)),
                dma((2, 2)),
                dma((KEEP, 2)),
                dma((groups, 2)),
                dma((KEEP, 2)),
                dma((groups, 2)),
                dma((KEEP, 2)),
                dma((KEEP, 2)),
            ],
            compiler_params=pltpu.CompilerParams(
                collective_id=0, has_side_effects=True, vmem_limit_bytes=40 * 1024 * 1024
            ),
            name="sums",
        )(a, g)[0]

        def write(begin, end_even, end_odd, *args):
            return pl.pallas_call(
                functools.partial(write_kernel, per, begin, end_even, end_odd),
                out_shape=(jax.ShapeDtypeStruct((count, d, ff), BF16), token),
                in_specs=[vmem, hbm][: len(args)],
                out_specs=(hbm, hbm),
                input_output_aliases={1: 0} if begin else {},
                scratch_shapes=[dma((groups,))],
                compiler_params=pltpu.CompilerParams(vmem_limit_bytes=4 * 1024 * 1024),
                name=f"write{begin}",
            )(*args)

        split = groups - LATER
        out, done = write(0, groups, split, res)
        later = pl.pallas_call(
            functools.partial(later_kernel, per, groups),
            out_shape=pltpu.VMEM((LATER, d, GROUP * WIDTH), BF16),
            in_specs=[vmem, hbm],
            out_specs=vmem,
            scratch_shapes=[dma((LATER, 2))] * 4 + [dma((LATER,))],
            compiler_params=pltpu.CompilerParams(
                collective_id=1, has_side_effects=True, vmem_limit_bytes=4 * 1024 * 1024
            ),
            name="later",
        )(res, done)
        return write(split, split, groups, later, out)[0]

    return jax.shard_map(
        local,
        mesh=mesh,
        in_specs=(P(("rep", "dp")), P(("rep", "dp"))),
        out_specs=P("rep"),
        check_vma=False,
    )
```

```python
import functools

import jax
import jax.numpy as jnp
from jax import lax
from jax.experimental import pallas as pl
from jax.experimental.pallas import tpu as pltpu
from jax.sharding import PartitionSpec as P

MESH = pl.DeviceIdType.MESH
BF16 = jnp.bfloat16
WIDTH = 256
GROUP = 3
FIRST = 4
T1, T2, T3, T4 = 3, 4, 6, 7
EVERY, OFFSET = 4, 9
LATER = 2
DEEP = 3
FWD = 2
ACC, V1, V2, SEND = T4 + 1, T4 - T1 + 1, T4 - T3 + 1, 4
RECV, KEEP = 7, 4


def sums_kernel(per, pieces, a_ref, g_ref, res, land, h1, h2, a_buf, g_buf, acc, sb1, sb2, v1, v2,
                a_sem, g_sem, f_sem, s1s, s1r, s2s, s2r, l1, l2, ags, agr, fws, fwr, lon, lof):
    n = 4
    me = lax.axis_index("dp")
    right, left, opp = lax.rem(me + 1, n), lax.rem(me + 3, n), lax.rem(me + 2, n)
    sides = (right, left)
    rows = h1.shape[2]
    half = rows // 2
    odd = lax.rem(lax.axis_index("rep"), 2)
    groups = pieces // GROUP - odd * LATER
    chunk = a_buf.shape[1] // FIRST

    def rows_of(owner, h=None):
        start = owner * rows + (0 if h is None else h * half)
        return pl.ds(pl.multiple_of(start, 16), rows if h is None else half)

    def block(ref, p, width, owner, h=None):
        m, q = lax.div(p, per), lax.rem(p, per)
        return ref.at[m, rows_of(owner, h), pl.ds(pl.multiple_of(q * WIDTH, WIDTH), width)]

    def load_a(m):
        return pltpu.make_async_copy(a_ref.at[0, m], a_buf.at[lax.rem(m, 2)], a_sem.at[lax.rem(m, 2)])

    def load_g(p):
        m, q = lax.div(p, per), lax.rem(p, per)
        slot = lax.rem(p, 3)
        cols = pl.ds(pl.multiple_of(q * WIDTH, WIDTH), WIDTH)
        return pltpu.make_async_copy(g_ref.at[0, m, :, cols], g_buf.at[slot], g_sem.at[slot])

    def first(k):
        t = pl.ds(pl.multiple_of(k * chunk, chunk), chunk)
        return (
            pltpu.make_async_copy(g_ref.at[0, 0, t, pl.ds(0, WIDTH)], g_buf.at[0, t], f_sem.at[k, 0]),
            pltpu.make_async_copy(a_ref.at[0, 0, t], a_buf.at[0, t], f_sem.at[k, 1]),
        )

    def remote(src, dst, ss, rs, d):
        return pltpu.make_async_remote_copy(
            src_ref=src, dst_ref=dst, send_sem=ss, recv_sem=rs, device_id={"dp": sides[d]}, device_id_type=MESH
        )

    def send1(p, d):
        slot = lax.rem(p, SEND)
        return remote(sb1.at[slot, d], h1.at[p, d], s1s.at[slot, d], s1r.at[lax.rem(p, RECV), d], d)

    def send2(p, d):
        slot = lax.rem(p, SEND)
        return remote(sb2.at[slot, d], h2.at[p, d], s2s.at[slot, d], s2r.at[lax.rem(p, RECV), d], d)

    def load1(p, d):
        slot = lax.rem(p, V1)
        return pltpu.make_async_copy(h1.at[p, d], v1.at[slot, d], l1.at[lax.rem(p, 2), d])

    def load2(p, d):
        slot = lax.rem(p, V2)
        return pltpu.make_async_copy(h2.at[p, d], v2.at[slot, d], l2.at[lax.rem(p, 2), d])

    def gather(k, d):
        b = block(land, k * GROUP, GROUP * WIDTH, me)
        return remote(block(res, k * GROUP, GROUP * WIDTH, me), b, ags.at[lax.rem(k, KEEP), d], agr.at[k, d], d)

    def forward(k, d, to):
        p, width, owner = k * GROUP, GROUP * WIDTH, (left, right)[d]
        return remote(
            block(land, p, width, owner, d), block(to, p, width, owner, d), fws.at[lax.rem(k, KEEP), d], fwr.at[k, d], d
        )

    def keep_near(k, d):
        p, width, owner = k * GROUP, GROUP * WIDTH, (left, right)[d]
        return pltpu.make_async_copy(
            block(land, p, width, owner), block(res, p, width, owner), lon.at[lax.rem(k, KEEP), d]
        )

    def keep_far(k, d):
        p, width = k * GROUP, GROUP * WIDTH
        return pltpu.make_async_copy(
            block(land, p, width, opp, d), block(res, p, width, opp, d), lof.at[lax.rem(k, KEEP), d]
        )

    def gather_start(k):
        @pl.when(k >= KEEP)
        def _():
            for d in range(2):
                gather(k - KEEP, d).wait_send()

        for d in range(2):
            gather(k, d).start()

    def forward_start(k, to=land):
        @pl.when(k >= KEEP)
        def _():
            for d in range(2):
                forward(k - KEEP, d, land).wait_send()
                keep_near(k - KEEP, d).wait()

        for d in range(2):
            gather(k, d).wait_recv()
            forward(k, d, to).start()
            keep_near(k, d).start()

    def far_start(k):
        @pl.when(k >= KEEP)
        def _():
            for d in range(2):
                keep_far(k - KEEP, d).wait()

        for d in range(2):
            forward(k, d, land).wait_recv()
            keep_far(k, d).start()

    for k in range(FIRST):
        for copy in first(k)[::-1]:
            copy.start()
    load_g(1).start()

    barrier = pltpu.get_barrier_semaphore()
    for d in sides:
        pl.semaphore_signal(barrier, inc=1, device_id={"dp": d}, device_id_type=MESH)

    def product(lhs, rhs):
        return lax.dot_general(lhs, rhs, (((0,), (0,)), ((), ())), preferred_element_type=jnp.float32)

    acc[0] = jnp.zeros_like(acc[0])

    def first_step(k, carry):
        for copy in first(k):
            copy.wait()
        t = pl.ds(pl.multiple_of(k * chunk, chunk), chunk)
        acc[0] += product(a_buf[0, t], g_buf[0, t])
        return carry

    lax.fori_loop(0, FIRST, first_step, 0)
    pl.semaphore_wait(barrier, 2)

    def step(i, carry):
        @pl.when(i < pieces)
        def _():
            m, q = lax.div(i, per), lax.rem(i, per)
            slot, mine = lax.rem(i, SEND), lax.rem(i, ACC)

            @pl.when(i + 2 < pieces)
            def _():
                load_g(i + 2).start()

            @pl.when((q == 0) & (i + per < pieces))
            def _():
                load_a(m + 1).start()

            @pl.when(i > 0)
            def _():
                @pl.when(q == 0)
                def _():
                    load_a(m).wait()

                load_g(i).wait()
                acc[mine] = product(a_buf[lax.rem(m, 2)], g_buf[lax.rem(i, 3)])

            @pl.when(i >= SEND)
            def _():
                for d in range(2):
                    send1(i - SEND, d).wait_send()

            for d in range(2):
                sb1[slot, d, :half] = acc[mine, rows_of(opp, d)].astype(BF16)
                sb1[slot, d, half:] = acc[mine, rows_of(sides[d], 1 - d)].astype(BF16)
            for d in range(2):
                send1(i, d).start()

        @pl.when((i >= T1) & (i < pieces + T1))
        def _():
            for d in range(2):
                send1(i - T1, d).wait_recv()
                load1(i - T1, d).start()

        @pl.when((i >= T2) & (i < pieces + T2))
        def _():
            p = i - T2
            slot, mine, here = lax.rem(p, SEND), lax.rem(p, ACC), lax.rem(p, V1)

            @pl.when(p >= SEND)
            def _():
                for d in range(2):
                    send2(p - SEND, d).wait_send()

            for d in range(2):
                load1(p, d).wait()
                sb2[slot, d] = (acc[mine, rows_of(sides[d], d)] + v1[here, d, :half].astype(jnp.float32)).astype(BF16)
            for d in range(2):
                send2(p, d).start()

        @pl.when((i >= T3) & (i < pieces + T3))
        def _():
            for d in range(2):
                send2(i - T3, d).wait_recv()
                load2(i - T3, d).start()

        @pl.when(i >= T4)
        def _():
            p = i - T4
            m, q = lax.div(p, per), lax.rem(p, per)
            mine, one, two = lax.rem(p, ACC), lax.rem(p, V1), lax.rem(p, V2)
            cols = pl.ds(pl.multiple_of(q * WIDTH, WIDTH), WIDTH)
            for d in range(2):
                load2(p, d).wait()
                res[m, rows_of(me, d), cols] = (
                    acc[mine, rows_of(me, d)]
                    + v2[two, d].astype(jnp.float32)
                    + v1[one, 1 - d, half:].astype(jnp.float32)
                ).astype(BF16)

        t = i - OFFSET

        @pl.when((t >= 0) & (lax.rem(t, EVERY) == 0))
        def _():
            gather_start(lax.div(t, EVERY))

        @pl.when((t >= FWD) & (lax.rem(t - FWD, EVERY) == 0))
        def _():
            k = lax.div(t - FWD, EVERY)
            forward_start(k)

            @pl.when(k >= 2)
            def _():
                far_start(k - 2)

        return carry

    last = pieces + T4
    lax.fori_loop(0, last, step, 0)

    def over(f, start, stop):
        def body(k, carry):
            f(k)
            return carry

        lax.fori_loop(start, stop, body, 0)

    gathered = (last - 1 - OFFSET) // EVERY + 1
    forwarded = (last - 1 - OFFSET - FWD) // EVERY + 1
    kept = max(forwarded - 2, 0)
    final = groups - 1

    def tail(t):
        @pl.when((t >= gathered) & (t < groups))
        def _():
            gather_start(t)

        @pl.when((t - DEEP >= forwarded) & (t - DEEP < final))
        def _():
            forward_start(t - DEEP)

        @pl.when(t - DEEP == final)
        def _():
            forward_start(final, res)

        @pl.when((t - DEEP - 2 >= kept) & (t - DEEP - 2 < final))
        def _():
            far_start(t - DEEP - 2)

    over(tail, min(gathered, forwarded + DEEP, kept + DEEP + 2), groups + DEEP + 2)

    for p in range(pieces - SEND, pieces):
        for d in range(2):
            send1(p, d).wait_send()
            send2(p, d).wait_send()

    def drain(k):
        for d in range(2):
            gather(k, d).wait_send()
            keep_near(k, d).wait()
            forward(k, d, land).wait_send()

    def drain_far(k):
        for d in range(2):
            keep_far(k, d).wait()

    over(drain, groups - KEEP, groups)
    over(drain_far, final - KEEP, final)
    for d in range(2):
        forward(final, d, res).wait_recv()


def later_kernel(per, groups, res, after, land, sg, rg, sf, rf):
    n = 4
    odd = lax.rem(lax.axis_index("rep"), 2)
    me = lax.axis_index("dp")
    right, left = lax.rem(me + 1, n), lax.rem(me + 3, n)
    sides = (right, left)
    rows = res.shape[1] // n
    half = rows // 2

    def rows_of(owner, h=0, size=rows):
        return pl.ds(pl.multiple_of(owner * rows + h * half, 16), size)

    def own(k):
        p = (groups - LATER + k) * GROUP
        return res.at[p // per, rows_of(me), pl.ds(p % per * WIDTH, GROUP * WIDTH)]

    def remote(src, dst, ss, rs, d):
        return pltpu.make_async_remote_copy(
            src_ref=src, dst_ref=dst, send_sem=ss, recv_sem=rs, device_id={"dp": sides[d]}, device_id_type=MESH
        )

    def gather(k, d):
        return remote(own(k), land.at[k, rows_of(me)], sg.at[k, d], rg.at[k, d], d)

    def forward(k, d):
        b = land.at[k, rows_of((left, right)[d], d, half)]
        return remote(b, b, sf.at[k, d], rf.at[k, d], d)

    @pl.when(odd == 1)
    def _():
        barrier = pltpu.get_barrier_semaphore()
        for d in sides:
            pl.semaphore_signal(barrier, inc=1, device_id={"dp": d}, device_id_type=MESH)
        pl.semaphore_wait(barrier, 2)
        every = [(k, d) for k in range(LATER) for d in range(2)]
        for k, d in every:
            gather(k, d).start()
        for k, d in every:
            gather(k, d).wait_recv()
            forward(k, d).start()
        for k, d in every:
            gather(k, d).wait_send()
            forward(k, d).wait()


def write_kernel(per, begin, end_even, end_odd, res, *rest):
    o_ref, done, sem = rest[-3:]
    odd = lax.rem(lax.axis_index("rep"), 2)
    end = (1 - odd) * end_even + odd * end_odd

    def copy(k):
        p = k * GROUP
        cols = pl.ds(p % per * WIDTH, GROUP * WIDTH)
        if not begin:
            return [pltpu.make_async_copy(res.at[p // per, :, cols], o_ref.at[p // per, :, cols], sem.at[k, 0])]
        step = o_ref.shape[1] // 4
        me = lax.axis_index("dp")
        return [
            pltpu.make_async_copy(res.at[k - begin, rows], o_ref.at[p // per, rows, cols], sem.at[k, j])
            for j in range(3)
            for rows in [pl.ds(pl.multiple_of(lax.rem(me + 1 + j, 4) * step, 16), step)]
        ]

    for k in range(begin, max(end_even, end_odd)):
        @pl.when(k < end)
        def _():
            for one in copy(k):
                one.start()

    for k in range(begin, max(end_even, end_odd)):
        @pl.when(k < end)
        def _():
            for one in copy(k):
                one.wait()


def solution(mesh):
    def local(a, g):
        _, count, tokens, d = a.shape
        ff = g.shape[3]
        per = ff // WIDTH
        pieces = count * per
        rows = d // mesh.shape["dp"]
        groups = pieces // GROUP
        dma = pltpu.SemaphoreType.DMA
        vmem = pl.BlockSpec(memory_space=pltpu.VMEM)
        hbm = pl.BlockSpec(memory_space=pltpu.HBM)
        token = jax.ShapeDtypeStruct((8, 128), BF16)
        res = pl.pallas_call(
            functools.partial(sums_kernel, per, pieces),
            out_shape=(
                pltpu.VMEM((count, d, ff), BF16),
                jax.ShapeDtypeStruct((count, d, ff), BF16),
                jax.ShapeDtypeStruct((pieces, 2, rows, WIDTH), BF16),
                jax.ShapeDtypeStruct((pieces, 2, rows // 2, WIDTH), BF16),
            ),
            in_specs=[hbm] * 2,
            out_specs=(vmem, hbm, hbm, hbm),
            scratch_shapes=[
                pltpu.VMEM((2, tokens, d), BF16),
                pltpu.VMEM((3, tokens, WIDTH), BF16),
                pltpu.VMEM((ACC, d, WIDTH), jnp.float32),
                pltpu.VMEM((SEND, 2, rows, WIDTH), BF16),
                pltpu.VMEM((SEND, 2, rows // 2, WIDTH), BF16),
                pltpu.VMEM((V1, 2, rows, WIDTH), BF16),
                pltpu.VMEM((V2, 2, rows // 2, WIDTH), BF16),
                dma((2,)),
                dma((3,)),
                dma((FIRST, 2)),
                dma((SEND, 2)),
                dma((RECV, 2)),
                dma((SEND, 2)),
                dma((RECV, 2)),
                dma((2, 2)),
                dma((2, 2)),
                dma((KEEP, 2)),
                dma((groups, 2)),
                dma((KEEP, 2)),
                dma((groups, 2)),
                dma((KEEP, 2)),
                dma((KEEP, 2)),
            ],
            compiler_params=pltpu.CompilerParams(
                collective_id=0, has_side_effects=True, vmem_limit_bytes=40 * 1024 * 1024
            ),
            name="sums",
        )(a, g)[0]

        def write(begin, end_even, end_odd, *args):
            return pl.pallas_call(
                functools.partial(write_kernel, per, begin, end_even, end_odd),
                out_shape=(jax.ShapeDtypeStruct((count, d, ff), BF16), token),
                in_specs=[vmem, hbm][: len(args)],
                out_specs=(hbm, hbm),
                input_output_aliases={1: 0} if begin else {},
                scratch_shapes=[dma((groups, 3))],
                compiler_params=pltpu.CompilerParams(vmem_limit_bytes=4 * 1024 * 1024),
                name=f"write{begin}",
            )(*args)

        split = groups - LATER
        out, done = write(0, groups, groups, res)
        later = pl.pallas_call(
            functools.partial(later_kernel, per, groups),
            out_shape=pltpu.VMEM((LATER, d, GROUP * WIDTH), BF16),
            in_specs=[vmem, hbm],
            out_specs=vmem,
            scratch_shapes=[dma((LATER, 2))] * 4,
            compiler_params=pltpu.CompilerParams(
                collective_id=1, has_side_effects=True, vmem_limit_bytes=4 * 1024 * 1024
            ),
            name="later",
        )(res, done)
        return write(split, split, groups, later, out)[0]

    return jax.shard_map(
        local,
        mesh=mesh,
        in_specs=(P(("rep", "dp")), P(("rep", "dp"))),
        out_specs=P("rep"),
        check_vma=False,
    )
```
